32 devices in a mesh: dp: 1 (over z), hp: 4 (over y), sp: 8 (over x, core).
Axes of the slice: x: 4, y: 4, z: 1, core: 2. Of those that a mesh axis runs over, the one named last changes fastest.
The devices are a block of a 4x4x8 slice.
Arguments:
- tokens: bfloat16 [4, 1024, 2048], P('dp', 'sp')
- theta_q: bfloat16 [2048, 2048], P(None, 'hp')
- theta_k: bfloat16 [2048, 2048], P(None, 'hp')
- theta_v: bfloat16 [2048, 2048], P(None, 'hp')
- w_out: bfloat16 [2048, 2048], P('hp')
- w_one: float32 [16, 128, 512], P('hp')
- b_one: float32 [16, 512], P('hp')
- w_two: float32 [16, 512, 128], P('hp')
- b_two: float32 [16, 128], P('hp')
- ln_gamma: float32 [16, 128], P('hp')
- ln_beta: float32 [16, 128], P('hp')
- inner_lr: float32 [16], P('hp')
Outputs:
- output: bfloat16 [4, 1024, 2048], P('dp', 'sp', 'hp')
All inputs are finite; a program needn't handle non-finite values.
Results may differ from the reference program's by a relative error of at most 0.00195.
Values are sent between devices in bfloat16 or wider.
A program may use at most 768 MiB of HBM per device.

```python
import jax
import jax.numpy as jnp
from jax import lax

BATCH = 4
SEQ_LEN = 1024
MODEL_DIM = 2048
HEADS = 16
HEAD_DIM = 128
MINI_BATCH = 16
EPS = 1e-6
HIDDEN_DIM = 4 * HEAD_DIM
WIDTH = HEADS * HEAD_DIM


def setup_inputs(seed: int = 0, part: int = 0) -> dict:
    key_list = jax.random.split(jax.random.key(seed), 12)
    tok_key = jax.random.fold_in(key_list[0], part)
    tokens = jax.random.normal(tok_key, (BATCH, SEQ_LEN, MODEL_DIM), jnp.float32)
    proj_scale = MODEL_DIM ** -0.5

    def normal_draw(index, shape, scale):
        return jax.random.normal(key_list[index], shape, jnp.float32) * scale

    return {
        "tokens": tokens.astype(jnp.bfloat16),
        "theta_q": normal_draw(1, (MODEL_DIM, WIDTH), proj_scale).astype(jnp.bfloat16),
        "theta_k": normal_draw(2, (MODEL_DIM, WIDTH), proj_scale).astype(jnp.bfloat16),
        "theta_v": normal_draw(3, (MODEL_DIM, WIDTH), proj_scale).astype(jnp.bfloat16),
        "w_out": normal_draw(4, (WIDTH, MODEL_DIM), WIDTH ** -0.5).astype(jnp.bfloat16),
        "w_one": normal_draw(5, (HEADS, HEAD_DIM, HIDDEN_DIM), HEAD_DIM ** -0.5),
        "b_one": normal_draw(6, (HEADS, HIDDEN_DIM), 0.5),
        "w_two": normal_draw(7, (HEADS, HIDDEN_DIM, HEAD_DIM), HIDDEN_DIM ** -0.5),
        "b_two": normal_draw(8, (HEADS, HEAD_DIM), 0.5),
        "ln_gamma": 0.8 + 0.4 * jax.random.uniform(key_list[9], (HEADS, HEAD_DIM), jnp.float32),
        "ln_beta": normal_draw(10, (HEADS, HEAD_DIM), 0.3),
        "inner_lr": (0.1 + 0.2 * jax.random.uniform(key_list[11], (HEADS,), jnp.float32)) / HEAD_DIM,
    }


def inner_apply(params, norm_gain, norm_bias, inputs):
    w_first, b_first, w_second, b_second = params
    hidden = jax.nn.gelu(jnp.dot(inputs, w_first, precision=lax.Precision.HIGHEST) + b_first)
    pre_norm = jnp.dot(hidden, w_second, precision=lax.Precision.HIGHEST) + b_second
    centered = pre_norm - jnp.mean(pre_norm, axis=-1, keepdims=True)
    variance = jnp.mean(centered * centered, axis=-1, keepdims=True)
    return inputs + norm_gain * centered * lax.rsqrt(variance + EPS) + norm_bias


def head_step(params, block, norm_gain, norm_bias, step_size):
    key_blk, value_blk, query_blk = [part_blk.astype(jnp.float32) for part_blk in block]

    def recon_loss(weights):
        residual = inner_apply(weights, norm_gain, norm_bias, key_blk) - value_blk
        return jnp.sum(residual * residual)

    gradients = jax.grad(recon_loss)(params)
    factor = step_size / MINI_BATCH
    updated = tuple(tensor - factor * grad_val for tensor, grad_val in zip(params, gradients))
    return updated, inner_apply(updated, norm_gain, norm_bias, query_blk)


batch_step = jax.vmap(jax.vmap(head_step), in_axes=(0, 0, None, None, None))


def reference(tokens, theta_q, theta_k, theta_v, w_out, w_one, b_one, w_two, b_two, ln_gamma, ln_beta, inner_lr):
    n_blocks = SEQ_LEN // MINI_BATCH
    flat_tok = tokens.reshape(BATCH * SEQ_LEN, MODEL_DIM)

    def project(weight):
        projected = jnp.dot(flat_tok, weight, preferred_element_type=jnp.float32).astype(jnp.bfloat16)
        return jnp.transpose(projected.reshape(BATCH, n_blocks, MINI_BATCH, HEADS, HEAD_DIM), (1, 0, 3, 2, 4))

    blocks = (project(theta_k), project(theta_v), project(theta_q))
    start = tuple(jnp.broadcast_to(tensor, (BATCH,) + tensor.shape) for tensor in (w_one, b_one, w_two, b_two))

    def body(state, block):
        return batch_step(state, block, ln_gamma, ln_beta, inner_lr)

    head_out = lax.scan(body, start, blocks)[1]
    head_out = head_out.astype(jnp.bfloat16).astype(jnp.float32)
    mixed = jnp.einsum("nbhme,hed->bnmd", head_out, w_out.reshape(HEADS, HEAD_DIM, MODEL_DIM).astype(jnp.float32))
    return mixed.reshape(BATCH, SEQ_LEN, MODEL_DIM).astype(jnp.bfloat16)
```

```python
import functools

import jax
import jax.numpy as jnp
from jax import lax
from jax.experimental import pallas as pl
from jax.experimental.pallas import tpu as pltpu
from jax.sharding import PartitionSpec as P

MINI = 16
EPS = 1e-6
GELU_A = 0.7978845608028654
GELU_B = 0.044715
F32 = jnp.float32
BF16 = jnp.bfloat16


def split3(x):
    high = x.astype(BF16)
    rest = x - high.astype(F32)
    mid = rest.astype(BF16)
    low = (rest - mid.astype(F32)).astype(BF16)
    return high, mid, low


def dot(a, b):
    return jnp.dot(a, b, preferred_element_type=F32)


def dot_t(a, b):
    return lax.dot_general(a, b, (((1,), (1,)), ((), ())), preferred_element_type=F32)


def six(parts):
    high, mid, low = parts
    return [high, mid, low, high, mid, high]


def six_other(parts):
    high, mid, low = parts
    return [high, high, high, mid, mid, low]


def ttt_kernel(n_chains, kvq, w1, b1, w2, b2, gamma, beta, rate, out, *scr):
    n_blocks, block = kvq.shape[0], kvq.shape[3]
    per_block = block // MINI
    n_steps = n_blocks * per_block
    dim, hid = w1.shape
    per = len(scr) // n_chains
    chains = [scr[i * per:(i + 1) * per] for i in range(n_chains)]
    factor = rate[0, 0] / MINI
    gain, bias = gamma[...], beta[...]

    def load(chain, which, step):
        return kvq[step // per_block, chain, which, pl.ds(pl.multiple_of((step % per_block) * MINI, MINI), MINI), :]

    def store_first(refs, value):
        w1f, w1hm, w1lo = refs
        high, mid, low = split3(value)
        w1f[...] = value
        w1hm[:dim] = high
        w1hm[dim:] = mid
        w1lo[...] = low

    def correction(x, keys):
        rep = jnp.concatenate([keys] * 8, axis=0)
        a = dot_t(x, rep) + 1.0
        high, mid, low = split3(a)
        lane = lax.broadcasted_iota(jnp.int32, a.shape, 1)
        part = jnp.where(lane < 3 * MINI, high.astype(F32), jnp.where(lane < 5 * MINI, mid.astype(F32), low.astype(F32)))
        return jnp.where(lane < 6 * MINI, part, 0.0).astype(BF16)

    def base(x, w1hm, w1lo, b1r):
        return dot(jnp.concatenate([x, x], axis=1), w1hm[...]) + dot(x, w1lo[...]) + b1r[...]

    zeros32 = jnp.zeros((2 * MINI, hid), BF16)

    for c in range(n_chains):
        w1f, w1hm, w1lo, w2f, w2hm, w2lo, b1r, b2r, zb, cor, dh8 = chains[c]
        store_first((w1f, w1hm, w1lo), w1[...])
        w2t = w2[...].T
        w2t = w2t - jnp.mean(w2t, axis=0, keepdims=True)
        store_first((w2f, w2hm, w2lo), w2t)
        b1r[...] = b1[...]
        b2r[...] = b2[...] - jnp.mean(b2[...], axis=1, keepdims=True)
        dh8[...] = jnp.zeros_like(dh8)
        cor[...] = jnp.zeros_like(cor)
        zb[...] = base(jnp.concatenate([load(c, 2, 0), load(c, 0, 0)], axis=0), w1hm, w1lo, b1r)

    def step_chain(c, step):
        w1f, w1hm, w1lo, w2f, w2hm, w2lo, b1r, b2r, zb, cor, dh8 = chains[c]
        after = jnp.minimum(step + 1, n_steps - 1)
        before = jnp.maximum(step - 1, 0)
        key, val, qry = load(c, 0, step), load(c, 1, step), load(c, 2, step)
        key_before, qry_before = load(c, 0, before), load(c, 2, before)
        key_f, val_f, qry_f = key.astype(F32), val.astype(F32), qry_before.astype(F32)

        z = zb[...] - dot(cor[...], dh8[...])
        yield

        keys_t = jnp.concatenate([key_before] * 3 + [jnp.zeros((5 * MINI, dim), BF16)], axis=0).T
        new_w1 = w1f[...] - dot(keys_t, dh8[...])
        store_first((w1f, w1hm, w1lo), new_w1)
        yield

        z2 = z * z
        t = jnp.tanh(z * (GELU_A + (GELU_A * GELU_B) * z2))
        cdf = 0.5 + 0.5 * t
        h = z * cdf
        zk, z2k, tk = z[MINI:], z2[MINI:], t[MINI:]
        slope = cdf[MINI:] + (0.5 * zk * (1.0 - tk * tk)) * (GELU_A + (3.0 * GELU_A * GELU_B) * z2k)
        hp = split3(h)
        r = dot_t(jnp.concatenate(hp, axis=0), w2hm[...])
        yl = dot_t(hp[0], w2lo[...])
        yield

        x_after = jnp.concatenate([qry, load(c, 0, after)], axis=0)
        zb[...] = base(x_after, w1hm, w1lo, b1r)
        cor[...] = correction(x_after, key)
        yield

        n2 = 2 * MINI
        r = r[:, :dim] + r[:, dim:]
        yc = r[:n2] + r[n2:2 * n2] + r[2 * n2:] + yl + b2r[...]
        var = jnp.mean(yc * yc, axis=1, keepdims=True)
        rstd = lax.rsqrt(var + EPS)
        xhat = yc * rstd
        out[before // per_block, c, pl.ds(pl.multiple_of((before % per_block) * MINI, MINI), MINI), :] = (
            qry_f + gain * xhat[:MINI] + bias).astype(BF16)

        xk = xhat[MINI:]
        dx = (key_f + gain * xk + bias - val_f) * ((2.0 * factor) * gain)
        m1 = jnp.mean(dx, axis=1, keepdims=True)
        m2 = jnp.mean(dx * xk, axis=1, keepdims=True)
        dy = rstd[MINI:] * (dx - m1 - xk * m2)
        dyp = split3(dy)
        d3 = jnp.concatenate(dyp, axis=0)
        e = dot(jnp.concatenate([d3, d3], axis=1), w2hm[...])
        el = dot(dyp[0], w2lo[...])
        yield

        hk8 = jnp.concatenate(six([p[MINI:] for p in hp]) + [zeros32], axis=0)
        dy_t = jnp.concatenate(six_other(dyp) + [jnp.zeros((2 * MINI, dim), BF16)], axis=0).T
        new_w2 = w2f[...] - dot(dy_t, hk8)
        store_first((w2f, w2hm, w2lo), new_w2)
        b2r[...] = b2r[...] - jnp.sum(dy, axis=0, keepdims=True)
        yield

        dh = (e[:MINI] + e[MINI:2 * MINI] + e[2 * MINI:] + el) * slope
        dhp = six(split3(dh))
        dh8[:6 * MINI] = jnp.concatenate(dhp, axis=0)
        b1r[...] = b1r[...] - jnp.sum(dh, axis=0, keepdims=True)

    def body(step, carry):
        running = [step_chain(c, step) for c in range(n_chains)]
        while running:
            running = [g for g in running if next(g, 1) is None]
        return carry

    lax.fori_loop(0, n_steps, body, 0)

    for c in range(n_chains):
        w1f, w1hm, w1lo, w2f, w2hm, w2lo, b1r, b2r, zb, cor, dh8 = chains[c]
        qry = load(c, 2, n_steps - 1)
        z = zb[:MINI] - dot(cor[...], dh8[...])[:MINI]
        t = jnp.tanh(z * (GELU_A + (GELU_A * GELU_B) * (z * z)))
        h = z * (0.5 + 0.5 * t)
        hp = split3(h)
        r = dot_t(jnp.concatenate(hp, axis=0), w2hm[...])
        r = r[:, :dim] + r[:, dim:]
        yc = r[:MINI] + r[MINI:2 * MINI] + r[2 * MINI:] + dot_t(hp[0], w2lo[...]) + b2r[...]
        xhat = yc * lax.rsqrt(jnp.mean(yc * yc, axis=1, keepdims=True) + EPS)
        out[n_blocks - 1, c, pl.ds(block - MINI, MINI), :] = (qry.astype(F32) + gain * xhat + bias).astype(BF16)


def run_chains(kvq, w1, b1, w2, b2, gamma, beta, rate):
    n_blocks, n_chains, _, block, dim = kvq.shape
    hid = w1.shape[1]
    vmem = pl.BlockSpec(memory_space=pltpu.VMEM)
    per_chain = [
        pltpu.VMEM((dim, hid), F32), pltpu.VMEM((2 * dim, hid), BF16), pltpu.VMEM((dim, hid), BF16),
        pltpu.VMEM((dim, hid), F32), pltpu.VMEM((2 * dim, hid), BF16), pltpu.VMEM((dim, hid), BF16),
        pltpu.VMEM((1, hid), F32), pltpu.VMEM((1, dim), F32), pltpu.VMEM((2 * MINI, hid), F32),
        pltpu.VMEM((2 * MINI, 8 * MINI), BF16), pltpu.VMEM((8 * MINI, hid), BF16),
    ]
    return pl.pallas_call(
        functools.partial(ttt_kernel, n_chains),
        out_shape=jax.ShapeDtypeStruct((n_blocks, n_chains, block, dim), BF16),
        in_specs=[vmem] * 7 + [pl.BlockSpec(memory_space=pltpu.SMEM)],
        out_specs=vmem,
        scratch_shapes=per_chain * n_chains,
    )(kvq, w1, b1, w2, b2, gamma, beta, rate)


def solution(mesh):
    sp = mesh.shape["sp"]
    hp = mesh.shape["hp"]

    def local_fn(tokens, theta_q, theta_k, theta_v, w_out, w_one, b_one, w_two, b_two, ln_gamma, ln_beta, inner_lr):
        batch, block, model = tokens.shape
        heads, dim = w_one.shape[0], w_one.shape[1]
        n_chains = heads * batch // sp
        flat = tokens.reshape(batch * block, model)

        def project(theta):
            p = jnp.dot(flat, theta, preferred_element_type=F32).astype(BF16)
            p = p.reshape(batch, block, heads, dim).transpose(2, 0, 1, 3)
            return p.reshape(sp, n_chains, 1, block, dim)

        kvq = jnp.concatenate([project(theta_k), project(theta_v), project(theta_q)], axis=2)
        kvq = lax.all_to_all(kvq, "sp", 0, 0, tiled=True)

        first = lax.axis_index("sp") * n_chains
        head = first // batch

        def pick(arr):
            return lax.dynamic_index_in_dim(arr, head, 0, keepdims=False)

        got = run_chains(kvq, pick(w_one), pick(b_one)[None], pick(w_two), pick(b_two)[None], pick(ln_gamma)[None],
                         pick(ln_beta)[None], pick(inner_lr).reshape(1, 1))
        got = lax.all_to_all(got, "sp", 0, 0, tiled=True)
        got = got.reshape(heads, batch, block, dim)
        got = lax.all_gather(got, "hp", axis=0, tiled=True)
        w_cols = lax.all_to_all(w_out, "hp", 1, 0, tiled=True)
        rows = got.transpose(1, 2, 0, 3).reshape(batch * block, hp * heads * dim)
        res = jnp.dot(rows, w_cols, preferred_element_type=F32).astype(BF16)
        return res.reshape(batch, block, model // hp)

    head_spec = P("hp", None)
    cube_spec = P("hp", None, None)
    col_spec = P(None, "hp")
    return jax.shard_map(local_fn, mesh=mesh, in_specs=(P("dp", "sp", None), col_spec, col_spec, col_spec, head_spec, cube_spec, head_spec, cube_spec, head_spec, head_spec, head_spec, P("hp")), out_specs=P("dp", "sp", "hp"), check_vma=False)
```

```python
import functools

import jax
import jax.numpy as jnp
from jax import lax
from jax.experimental import pallas as pl
from jax.experimental.pallas import tpu as pltpu
from jax.sharding import PartitionSpec as P

MINI = 16
EPS = 1e-6
GELU_A = 0.7978845608028654
GELU_B = 0.044715
F32 = jnp.float32
BF16 = jnp.bfloat16


def split3(x):
    high = x.astype(BF16)
    rest = x - high.astype(F32)
    mid = rest.astype(BF16)
    low = (rest - mid.astype(F32)).astype(BF16)
    return high, mid, low


def dot(a, b):
    return jnp.dot(a, b, preferred_element_type=F32)


def dot_t(a, b):
    return lax.dot_general(a, b, (((1,), (1,)), ((), ())), preferred_element_type=F32)


def six(parts):
    high, mid, low = parts
    return [high, mid, low, high, mid, high]


def six_other(parts):
    high, mid, low = parts
    return [high, high, high, mid, mid, low]


MESH = pl.DeviceIdType.MESH
PIECE = 2 * MINI
CHAIN_REFS = 11


def ttt_kernel(n_hp, n_sp, n_chains, tokens, theta_k, theta_v, theta_q, w_out, w_one, w_two, b_one, b_two, gammas, betas, rates,
               res, tok, theta, wcols, kvq, send, outb, gath, w1, w2, in_sem, send_sem, recv_sem, wsend_sem, wrecv_sem,
               osend_sem, orecv_sem, *scr):
    batch, block, model = tokens.shape
    heads, dim, hid = w_one.shape
    n_pieces = block // PIECE
    per_block = block // MINI
    per_piece = PIECE // MINI
    n_steps = n_sp * per_block
    cols = model // n_hp
    rows = heads * dim
    per_head = batch // n_chains
    my_hp, me = lax.axis_index("hp"), lax.axis_index("sp")
    linear = my_hp * n_sp + me
    n_all = n_hp * n_sp
    head = me // per_head
    chains = [scr[i * CHAIN_REFS:(i + 1) * CHAIN_REFS] for i in range(n_chains)]
    factor = rates[head] / MINI
    gain, bias = gammas[pl.ds(head, 1), :], betas[pl.ds(head, 1), :]

    def head_of(turn):
        return lax.rem(head + turn, heads)

    barrier = pltpu.get_barrier_semaphore()
    for off in range(1, n_all):
        other = lax.rem(linear + off, n_all)
        pl.semaphore_signal(barrier, inc=1, device_id={"hp": other // n_sp, "sp": lax.rem(other, n_sp)}, device_id_type=MESH)

    loads = []

    def fetch(src, dst):
        copy = pltpu.make_async_copy(src, dst, in_sem.at[len(loads)])
        copy.start()
        loads.append(copy)

    turns = [[2, 1], [3, 0]]
    for b in range(batch):
        fetch(tokens.at[b], tok.at[pl.ds(b * block, block)])
    for r, pair in enumerate(turns):
        for u, turn in enumerate(pair):
            where = pl.ds(pl.multiple_of(head_of(turn) * dim, dim), dim)
            for i, part in enumerate((theta_k, theta_v, theta_q)):
                fetch(part.at[:, where], theta.at[r, :, pl.ds((u * 3 + i) * dim, dim)])
    fetch(w_one.at[head], w1)
    fetch(w_two.at[head], w2)
    mine = pl.ds(pl.multiple_of(my_hp * cols, cols), cols)
    my_rows = pl.ds(pl.multiple_of(my_hp * rows, rows), rows)
    fetch(w_out.at[:, mine], wcols.at[my_rows])

    done = 0
    for r, pair in enumerate(turns):
        upto = batch + (r + 1) * 3 * len(pair)
        for copy in loads[done:upto]:
            copy.wait()
        done = upto
        p = dot(tok[...], theta[r]).astype(BF16)
        for u, turn in enumerate(pair):
            for b in range(batch):
                dest = head_of(turn) * per_head + b // n_chains
                for i in range(3):
                    tile = p[b * block:(b + 1) * block, (u * 3 + i) * dim:(u * 3 + i + 1) * dim]
                    for q in range(n_pieces):
                        send[dest, q, b % n_chains, i] = tile[q * PIECE:(q + 1) * PIECE]
    for copy in loads[done:]:
        copy.wait()
    kvq[me] = send[me]

    pl.semaphore_wait(barrier, n_all - 1)

    def kvq_copy(off, q):
        dest = lax.rem(me + off, n_sp)
        return pltpu.make_async_remote_copy(src_ref=send.at[dest, q], dst_ref=kvq.at[me, q], send_sem=send_sem.at[off, q],
                                            recv_sem=recv_sem.at[me, q], device_id={"sp": dest}, device_id_type=MESH)

    def send_all():
        for q in range(n_pieces):
            for off in range(1, n_sp):
                kvq_copy(off, q).start()

    def wait_piece(number):
        src, q = number // n_pieces, lax.rem(number, n_pieces)

        @pl.when(src != me)
        def _():
            pltpu.make_async_remote_copy(src_ref=send.at[0, q], dst_ref=kvq.at[src, q], send_sem=send_sem.at[0, q],
                                         recv_sem=recv_sem.at[src, q], device_id={"sp": src}, device_id_type=MESH).wait_recv()

    def w_copy(off):
        dest = lax.rem(my_hp + off, n_hp)
        return pltpu.make_async_remote_copy(
            src_ref=w_out.at[:, pl.ds(pl.multiple_of(dest * cols, cols), cols)], dst_ref=wcols.at[my_rows],
            send_sem=wsend_sem.at[off], recv_sem=wrecv_sem.at[off], device_id={"hp": dest}, device_id_type=MESH)

    @pl.when(me == 0)
    def _():
        send_all()

    for off in range(1, n_hp):
        w_copy(off).start()

    def send_out(number):
        dest, q = number // n_pieces, lax.rem(number, n_pieces)

        def start(off):
            target = lax.rem(my_hp + off, n_hp)
            pltpu.make_async_remote_copy(src_ref=outb.at[dest, q], dst_ref=gath.at[linear, q], send_sem=osend_sem,
                                         recv_sem=orecv_sem, device_id={"hp": target, "sp": dest}, device_id_type=MESH).start()

        for off in range(1, n_hp):
            start(off)

        @pl.when(dest != me)
        def _():
            start(0)

        @pl.when(dest == me)
        def _():
            gath[linear, q] = outb[dest, q]

    def load(chain, which, step):
        piece = lax.rem(step, per_block)
        return kvq[step // per_block, piece // per_piece, chain, which, pl.ds(pl.multiple_of(lax.rem(piece, per_piece) * MINI, MINI), MINI), :]

    def store_out(chain, step, value):
        piece = lax.rem(step, per_block)
        outb[step // per_block, piece // per_piece, chain, pl.ds(pl.multiple_of(lax.rem(piece, per_piece) * MINI, MINI), MINI), :] = value.astype(BF16)

    def store_first(refs, value):
        w1f, w1hm, w1lo = refs
        high, mid, low = split3(value)
        w1f[...] = value
        w1hm[:dim] = high
        w1hm[dim:] = mid
        w1lo[...] = low

    def correction(x, keys):
        rep = jnp.concatenate([keys] * 8, axis=0)
        a = dot_t(x, rep) + 1.0
        high, mid, low = split3(a)
        lane = lax.broadcasted_iota(jnp.int32, a.shape, 1)
        part = jnp.where(lane < 3 * MINI, high.astype(F32), jnp.where(lane < 5 * MINI, mid.astype(F32), low.astype(F32)))
        return jnp.where(lane < 6 * MINI, part, 0.0).astype(BF16)

    def base(x, w1hm, w1lo, b1r):
        return dot(jnp.concatenate([x, x], axis=1), w1hm[...]) + dot(x, w1lo[...]) + b1r[...]

    zeros32 = jnp.zeros((2 * MINI, hid), BF16)

    for c in range(n_chains):
        w1f, w1hm, w1lo, w2f, w2hm, w2lo, b1r, b2r, zb, cor, dh8 = chains[c]
        store_first((w1f, w1hm, w1lo), w1[...])
        w2t = w2[...].T
        w2t = w2t - jnp.mean(w2t, axis=0, keepdims=True)
        store_first((w2f, w2hm, w2lo), w2t)
        b1r[...] = b_one[pl.ds(head, 1), :]
        b2 = b_two[pl.ds(head, 1), :]
        b2r[...] = b2 - jnp.mean(b2, axis=1, keepdims=True)
        dh8[...] = jnp.zeros_like(dh8)
        cor[...] = jnp.zeros_like(cor)

    wait_piece(0)
    for c in range(n_chains):
        w1f, w1hm, w1lo, w2f, w2hm, w2lo, b1r, b2r, zb, cor, dh8 = chains[c]
        zb[...] = base(jnp.concatenate([load(c, 2, 0), load(c, 0, 0)], axis=0), w1hm, w1lo, b1r)

    def step_chain(c, step):
        w1f, w1hm, w1lo, w2f, w2hm, w2lo, b1r, b2r, zb, cor, dh8 = chains[c]
        after = jnp.minimum(step + 1, n_steps - 1)
        before = jnp.maximum(step - 1, 0)
        key, val, qry = load(c, 0, step), load(c, 1, step), load(c, 2, step)
        key_before, qry_before = load(c, 0, before), load(c, 2, before)
        key_f, val_f, qry_f = key.astype(F32), val.astype(F32), qry_before.astype(F32)

        z = zb[...] - dot(cor[...], dh8[...])
        yield

        keys_t = jnp.concatenate([key_before] * 3 + [jnp.zeros((5 * MINI, dim), BF16)], axis=0).T
        new_w1 = w1f[...] - dot(keys_t, dh8[...])
        store_first((w1f, w1hm, w1lo), new_w1)
        yield

        z2 = z * z
        t = jnp.tanh(z * (GELU_A + (GELU_A * GELU_B) * z2))
        cdf = 0.5 + 0.5 * t
        h = z * cdf
        zk, z2k, tk = z[MINI:], z2[MINI:], t[MINI:]
        slope = cdf[MINI:] + (0.5 * zk * (1.0 - tk * tk)) * (GELU_A + (3.0 * GELU_A * GELU_B) * z2k)
        hp = split3(h)
        r = dot_t(jnp.concatenate(hp, axis=0), w2hm[...])
        yl = dot_t(hp[0], w2lo[...])
        yield

        x_after = jnp.concatenate([qry, load(c, 0, after)], axis=0)
        zb[...] = base(x_after, w1hm, w1lo, b1r)
        cor[...] = correction(x_after, key)
        yield

        n2 = 2 * MINI
        r = r[:, :dim] + r[:, dim:]
        yc = r[:n2] + r[n2:2 * n2] + r[2 * n2:] + yl + b2r[...]
        var = jnp.mean(yc * yc, axis=1, keepdims=True)
        rstd = lax.rsqrt(var + EPS)
        xhat = yc * rstd
        store_out(c, before, qry_f + gain * xhat[:MINI] + bias)

        xk = xhat[MINI:]
        dx = (key_f + gain * xk + bias - val_f) * ((2.0 * factor) * gain)
        m1 = jnp.mean(dx, axis=1, keepdims=True)
        m2 = jnp.mean(dx * xk, axis=1, keepdims=True)
        dy = rstd[MINI:] * (dx - m1 - xk * m2)
        dyp = split3(dy)
        d3 = jnp.concatenate(dyp, axis=0)
        e = dot(jnp.concatenate([d3, d3], axis=1), w2hm[...])
        el = dot(dyp[0], w2lo[...])
        yield

        hk8 = jnp.concatenate(six([p[MINI:] for p in hp]) + [zeros32], axis=0)
        dy_t = jnp.concatenate(six_other(dyp) + [jnp.zeros((2 * MINI, dim), BF16)], axis=0).T
        new_w2 = w2f[...] - dot(dy_t, hk8)
        store_first((w2f, w2hm, w2lo), new_w2)
        b2r[...] = b2r[...] - jnp.sum(dy, axis=0, keepdims=True)
        yield

        dh = (e[:MINI] + e[MINI:2 * MINI] + e[2 * MINI:] + el) * slope
        dhp = six(split3(dh))
        dh8[:6 * MINI] = jnp.concatenate(dhp, axis=0)
        b1r[...] = b1r[...] - jnp.sum(dh, axis=0, keepdims=True)

    def body(step, carry):
        after = step + 1

        @pl.when((lax.rem(after, per_piece) == 0) & (after < n_steps))
        def _():
            wait_piece(after // per_piece)

        @pl.when((me > 0) & (step == jnp.maximum(me - 2, 0) * per_block))
        def _():
            send_all()

        @pl.when((lax.rem(step, per_piece) == 1) & (step > per_piece))
        def _():
            send_out((step - 1) // per_piece - 1)

        running = [step_chain(c, step) for c in range(n_chains)]
        while running:
            running = [g for g in running if next(g, 1) is None]
        return carry

    lax.fori_loop(0, n_steps, body, 0)

    for c in range(n_chains):
        w1f, w1hm, w1lo, w2f, w2hm, w2lo, b1r, b2r, zb, cor, dh8 = chains[c]
        qry = load(c, 2, n_steps - 1)
        z = zb[:MINI] - dot(cor[...], dh8[...])[:MINI]
        t = jnp.tanh(z * (GELU_A + (GELU_A * GELU_B) * (z * z)))
        h = z * (0.5 + 0.5 * t)
        hp = split3(h)
        r = dot_t(jnp.concatenate(hp, axis=0), w2hm[...])
        r = r[:, :dim] + r[:, dim:]
        yc = r[:MINI] + r[MINI:2 * MINI] + r[2 * MINI:] + dot_t(hp[0], w2lo[...]) + b2r[...]
        xhat = yc * lax.rsqrt(jnp.mean(yc * yc, axis=1, keepdims=True) + EPS)
        store_out(c, n_steps - 1, qry.astype(F32) + gain * xhat + bias)


    send_out(n_sp * n_pieces - 1)
    for off in range(1, n_hp):
        w_copy(off).wait()
    everyone = gath.at[pl.ds(0, n_all - 1)]
    pltpu.make_async_copy(everyone, everyone, orecv_sem).wait()
    total = None
    for two in range(n_hp * heads // 2):
        left = []
        for one in (2 * two, 2 * two + 1):
            parts = []
            for b in range(batch):
                chain = one * batch + b
                parts += [gath[chain // n_chains, q, chain % n_chains] for q in range(n_pieces)]
            left.append(jnp.concatenate(parts, axis=0))
        term = dot(jnp.concatenate(left, axis=1), wcols[pl.ds(two * 2 * dim, 2 * dim), :])
        total = term if total is None else total + term
    total = total.astype(BF16)
    for b in range(batch):
        res[b] = total[b * block:(b + 1) * block]
    pltpu.make_async_copy(everyone, everyone, osend_sem).wait()
    for q in range(n_pieces):
        for off in range(1, n_sp):
            kvq_copy(off, q).wait_send()


def run(n_hp, n_sp, tokens, theta_k, theta_v, theta_q, w_out, w_one, w_two, b_one, b_two, gammas, betas, rates):
    batch, block, model = tokens.shape
    heads, dim, hid = w_one.shape
    n_chains = heads * batch // n_sp
    assert batch % n_chains == 0 and heads % 2 == 0 and block % PIECE == 0
    n_pieces = block // PIECE
    n_all = n_hp * n_sp
    cols = model // n_hp
    any_ref, vmem = pl.BlockSpec(memory_space=pl.ANY), pl.BlockSpec(memory_space=pltpu.VMEM)
    dma, v = pltpu.SemaphoreType.DMA, pltpu.VMEM
    per_chain = [
        v((dim, hid), F32), v((2 * dim, hid), BF16), v((dim, hid), BF16),
        v((dim, hid), F32), v((2 * dim, hid), BF16), v((dim, hid), BF16),
        v((1, hid), F32), v((1, dim), F32), v((2 * MINI, hid), F32),
        v((2 * MINI, 8 * MINI), BF16), v((8 * MINI, hid), BF16),
    ]
    assert len(per_chain) == CHAIN_REFS
    scratch = [
        v((batch * block, model), BF16), v((2, model, heads // 2 * 3 * dim), BF16), v((n_hp * heads * dim, cols), BF16),
        v((n_sp, n_pieces, n_chains, 3, PIECE, dim), BF16), v((n_sp, n_pieces, n_chains, 3, PIECE, dim), BF16),
        v((n_sp, n_pieces, n_chains, PIECE, dim), BF16), v((n_all, n_pieces, n_chains, PIECE, dim), BF16),
        v((dim, hid), F32), v((hid, dim), F32),
        dma((batch + 3 * heads + 3,)), dma((n_sp, n_pieces)), dma((n_sp, n_pieces)), dma((n_hp,)), dma((n_hp,)), dma, dma,
    ] + per_chain * n_chains
    return pl.pallas_call(
        functools.partial(ttt_kernel, n_hp, n_sp, n_chains),
        out_shape=jax.ShapeDtypeStruct((batch, block, cols), BF16),
        in_specs=[any_ref] * 7 + [vmem] * 4 + [pl.BlockSpec(memory_space=pltpu.SMEM)],
        out_specs=vmem,
        scratch_shapes=scratch,
        compiler_params=pltpu.CompilerParams(collective_id=0, has_side_effects=True),
    )(tokens, theta_k, theta_v, theta_q, w_out, w_one, w_two, b_one, b_two, gammas, betas, rates)


def solution(mesh):
    n_sp = mesh.shape["sp"]
    n_hp = mesh.shape["hp"]

    def local_fn(tokens, theta_q, theta_k, theta_v, w_out, w_one, b_one, w_two, b_two, ln_gamma, ln_beta, inner_lr):
        return run(n_hp, n_sp, tokens, theta_k, theta_v, theta_q, w_out, w_one, w_two, b_one, b_two, ln_gamma, ln_beta, inner_lr)

    head_spec = P("hp", None)
    cube_spec = P("hp", None, None)
    col_spec = P(None, "hp")
    return jax.shard_map(local_fn, mesh=mesh, in_specs=(P("dp", "sp", None), col_spec, col_spec, col_spec, head_spec, cube_spec, head_spec, cube_spec, head_spec, head_spec, head_spec, P("hp")), out_specs=P("dp", "sp", "hp"), check_vma=False)
```

```python
import functools

import jax
import jax.numpy as jnp
from jax import lax
from jax.experimental import pallas as pl
from jax.experimental.pallas import tpu as pltpu
from jax.sharding import PartitionSpec as P

MINI = 16
EPS = 1e-6
GELU_A = 0.7978845608028654
GELU_B = 0.044715
F32 = jnp.float32
BF16 = jnp.bfloat16


def split3(x):
    high = x.astype(BF16)
    rest = x - high.astype(F32)
    mid = rest.astype(BF16)
    low = (rest - mid.astype(F32)).astype(BF16)
    return high, mid, low


def dot(a, b):
    return jnp.dot(a, b, preferred_element_type=F32)


def dot_t(a, b):
    return lax.dot_general(a, b, (((1,), (1,)), ((), ())), preferred_element_type=F32)


def six(parts):
    high, mid, low = parts
    return [high, mid, low, high, mid, high]


def six_other(parts):
    high, mid, low = parts
    return [high, high, high, mid, mid, low]


MESH = pl.DeviceIdType.MESH
PIECE = 2 * MINI
CHAIN_REFS = 14
TURNS = [[2, 1], [3, 0]]
ORDER = ("A corr", "B y", "A w2", "B base", "A gelu", "A w1", "B ln", "A y", "B dh", "B w2", "A base", "B end", "A ln",
         "B corr", "B w1", "A dh", "B gelu", "A end")
PACE = 4
SHARE_LAG = 14
GROUP_LAG = 28
DIRECT = 2
W_STEP = 0


def ttt_kernel(n_hp, n_sp, n_chains, tokens, theta_k, theta_v, theta_q, w_out, w_one, w_two, b_one, b_two, gammas, betas, rates,
               res, tok, theta, wcols, kvq, send, outb, gath, made, resb, w1, w2, in_sem, send_sem, recv_sem, wsend_sem,
               wrecv_sem, osend_sem, orecv_sem, ssend_sem, srecv_sem, rsend_sem, rrecv_sem, ready_sem, *scr):
    batch, block, model = tokens.shape
    heads, dim, hid = w_one.shape
    n_pieces = block // PIECE
    per_block = block // MINI
    per_piece = PIECE // MINI
    n_steps = n_sp * per_block
    cols = model // n_hp
    rows = heads * dim
    per_head = batch // n_chains
    my_hp, me = lax.axis_index("hp"), lax.axis_index("sp")
    linear = my_hp * n_sp + me
    n_all = n_hp * n_sp
    head = me // per_head
    chains = [scr[i * CHAIN_REFS:(i + 1) * CHAIN_REFS] for i in range(n_chains)]
    factor = rates[head] / MINI
    gain, bias = gammas[pl.ds(head, 1), :], betas[pl.ds(head, 1), :]

    def head_of(turn):
        return lax.rem(head + turn, heads)

    barrier = pltpu.get_barrier_semaphore()
    for off in range(1, n_sp):
        pl.semaphore_signal(barrier, inc=1, device_id={"sp": lax.rem(me + off, n_sp)}, device_id_type=MESH)
    for off in range(1, n_hp):
        pl.semaphore_signal(barrier, inc=1, device_id={"hp": lax.rem(my_hp + off, n_hp)}, device_id_type=MESH)

    loads = []

    def fetch(src, dst):
        copy = pltpu.make_async_copy(src, dst, in_sem.at[len(loads)])
        copy.start()
        loads.append(copy)

    for b in range(batch):
        fetch(tokens.at[b], tok.at[pl.ds(b * block, block)])
    for r, pair in enumerate(TURNS):
        for u, turn in enumerate(pair):
            where = pl.ds(pl.multiple_of(head_of(turn) * dim, dim), dim)
            for i, part in enumerate((theta_k, theta_v, theta_q)):
                fetch(part.at[:, where], theta.at[r, :, pl.ds((u * 3 + i) * dim, dim)])
    fetch(w_one.at[head], w1)
    fetch(w_two.at[head], w2)
    mine = pl.ds(pl.multiple_of(my_hp * cols, cols), cols)
    my_rows = pl.ds(pl.multiple_of(my_hp * rows, rows), rows)
    fetch(w_out.at[:, mine], wcols.at[my_rows])

    half = n_sp // 2
    chip, core = me // 2, lax.rem(me, 2)

    def kvq_copy(delta, other, q, size):
        dest = lax.rem(chip + delta, half) * 2 + lax.rem(core + other, 2)
        return pltpu.make_async_remote_copy(
            src_ref=send.at[dest, pl.ds(q, size)], dst_ref=kvq.at[me, pl.ds(q, size)], send_sem=send_sem.at[2 * delta + other, q],
            recv_sem=recv_sem.at[me, q], device_id={"sp": dest}, device_id_type=MESH)

    kinds = [(me == 0, 1), (me == 1, 1), ((me > 1) & (me < half), 2), (me >= half, n_pieces)]

    def copies(which, deltas):
        size = kinds[which][1]
        return [kvq_copy(delta, other, q, size) for q in range(0, n_pieces, size) for delta in deltas for other in (0, 1)
                if delta + other > 0]

    def send_some(which, deltas, gate):
        @pl.when(kinds[which][0] & gate)
        def _():
            for copy in copies(which, deltas):
                copy.start()

    done = 0
    for r, pair in enumerate(TURNS):
        upto = batch + (r + 1) * 3 * len(pair)
        for copy in loads[done:upto]:
            copy.wait()
        done = upto
        p = dot(tok[...], theta[r]).astype(BF16)
        for u, turn in enumerate(pair):
            for b in range(batch):
                dest = head_of(turn) * per_head + b // n_chains
                for i in range(3):
                    tile = p[b * block:(b + 1) * block, (u * 3 + i) * dim:(u * 3 + i + 1) * dim]
                    for q in range(n_pieces):
                        send[dest, q, b % n_chains, i] = tile[q * PIECE:(q + 1) * PIECE]
        if r == 0:
            pl.semaphore_wait(barrier, n_sp + n_hp - 2)
            for off in range(1, n_hp):
                pl.semaphore_signal(ready_sem, inc=1, device_id={"hp": lax.rem(my_hp + off, n_hp)}, device_id_type=MESH)
        send_some(0, pair, me == 0)
    for copy in loads[done:]:
        copy.wait()
    kvq[me] = send[me]

    def wait_piece(number):
        src, q = number // n_pieces, lax.rem(number, n_pieces)

        def wait(size):
            pltpu.make_async_remote_copy(
                src_ref=send.at[0, pl.ds(q, size)], dst_ref=kvq.at[src, pl.ds(q, size)], send_sem=send_sem.at[0, q],
                recv_sem=recv_sem.at[src, q], device_id={"sp": src}, device_id_type=MESH).wait_recv()

        @pl.when((src != me) & (src < 2))
        def _():
            wait(1)

        @pl.when((src != me) & (src > 1) & (src < half) & (lax.rem(q, 2) == 0))
        def _():
            wait(2)

        @pl.when((src != me) & (src >= half) & (q == 0))
        def _():
            wait(n_pieces)

    def w_copy(off):
        dest = lax.rem(my_hp + off, n_hp)
        return pltpu.make_async_remote_copy(
            src_ref=w_out.at[:, pl.ds(pl.multiple_of(dest * cols, cols), cols)], dst_ref=wcols.at[my_rows],
            send_sem=wsend_sem.at[off], recv_sem=wrecv_sem.at[off], device_id={"hp": dest}, device_id_type=MESH)

    for off in range(1, n_hp):
        w_copy(off).start()

    def worker_of(turn):
        return lax.rem(turn, half) * 2 + turn // half

    my_turn = me // 2 + half * lax.rem(me, 2)
    n_groups = n_steps // per_piece // n_sp
    last = n_groups - 1
    first_direct = n_groups - DIRECT
    my_slots = pl.ds(pl.multiple_of(my_hp * n_sp, n_sp), n_sp)

    def send_out(number, spread):
        group, dest = number // n_sp, worker_of(lax.rem(number, n_sp))

        def start(off):
            target = lax.rem(my_hp + off, n_hp)
            pltpu.make_async_remote_copy(
                src_ref=outb.at[number], dst_ref=gath.at[group, linear], send_sem=osend_sem.at[int(spread)],
                recv_sem=orecv_sem.at[group], device_id={"hp": target, "sp": dest},
                device_id_type=MESH).start()

        if spread:
            for off in range(1, n_hp):
                start(off)

        @pl.when(dest != me)
        def _():
            start(0)

        @pl.when(dest == me)
        def _():
            gath[group, linear] = outb[number]

    def share_copy(group, off):
        return pltpu.make_async_remote_copy(
            src_ref=gath.at[group, my_slots], dst_ref=gath.at[group, my_slots], send_sem=ssend_sem, recv_sem=srecv_sem.at[group],
            device_id={"hp": lax.rem(my_hp + off, n_hp)}, device_id_type=MESH)

    def share_group(group):
        others = gath.at[group, pl.ds(0, n_sp - 1)]
        pltpu.make_async_copy(others, others, orecv_sem.at[group]).wait()
        for off in range(1, n_hp):
            share_copy(group, off).start()

    def result_copy(group):
        number = group * n_sp + my_turn
        owner, q = number // n_pieces, lax.rem(number, n_pieces)
        return owner, q, pltpu.make_async_remote_copy(
            src_ref=made.at[group], dst_ref=resb.at[q], send_sem=rsend_sem.at[group], recv_sem=rrecv_sem.at[q],
            device_id={"sp": owner}, device_id_type=MESH)

    def make_group(group):
        left = []
        for one in range(n_hp * heads):
            chain = [one * batch + b for b in range(batch)]
            left.append(jnp.concatenate([gath[group, c // n_chains, c % n_chains] for c in chain], axis=0))
        made[group] = dot(jnp.concatenate(left, axis=1), wcols[...]).astype(BF16).reshape(batch, PIECE, cols)
        owner, q, copy = result_copy(group)

        @pl.when(owner != me)
        def _():
            copy.start()

        @pl.when(owner == me)
        def _():
            resb[q] = made[group]

    def load(chain, which, step):
        piece = lax.rem(step, per_block)
        return kvq[step // per_block, piece // per_piece, chain, which, pl.ds(pl.multiple_of(lax.rem(piece, per_piece) * MINI, MINI), MINI), :]

    def store_out(chain, step, value):
        outb[step // per_piece, chain, pl.ds(pl.multiple_of(lax.rem(step, per_piece) * MINI, MINI), MINI), :] = value.astype(BF16)

    def store_first(refs, value):
        w1f, w1hm, w1lo = refs
        high, mid, low = split3(value)
        w1f[...] = value
        w1hm[:dim] = high
        w1hm[dim:] = mid
        w1lo[...] = low

    def correction(x, keys):
        rep = jnp.concatenate([keys] * 8, axis=0)
        a = dot_t(x, rep) + 1.0
        high, mid, low = split3(a)
        lane = lax.broadcasted_iota(jnp.int32, a.shape, 1)
        part = jnp.where(lane < 3 * MINI, high.astype(F32), jnp.where(lane < 5 * MINI, mid.astype(F32), low.astype(F32)))
        return jnp.where(lane < 6 * MINI, part, 0.0).astype(BF16)

    def base(x, w1hm, w1lo, b1r):
        return dot(jnp.concatenate([x, x], axis=1), w1hm[...]) + dot(x, w1lo[...]) + b1r[...]

    zeros32 = jnp.zeros((2 * MINI, hid), BF16)

    def hidden_in(c):
        return chains[c][8][...] - dot(chains[c][9][...], chains[c][10][...])

    def activate(c, z):
        w1f, w1hm, w1lo, w2f, w2hm, w2lo, b1r, b2r, zb, cor, dh8, hps, slope, d3r = chains[c]
        z2 = z * z
        t = jnp.tanh(z * (GELU_A + (GELU_A * GELU_B) * z2))
        cdf = 0.5 + 0.5 * t
        hps[...] = jnp.concatenate(split3(z * cdf), axis=0)
        zk, z2k, tk = z[MINI:], z2[MINI:], t[MINI:]
        slope[...] = cdf[MINI:] + (0.5 * zk * (1.0 - tk * tk)) * (GELU_A + (3.0 * GELU_A * GELU_B) * z2k)

    def update_first(c, step):
        w1f, w1hm, w1lo, w2f, w2hm, w2lo, b1r, b2r, zb, cor, dh8, hps, slope, d3r = chains[c]
        keys_t = jnp.concatenate([load(c, 0, step)] * 3 + [jnp.zeros((5 * MINI, dim), BF16)], axis=0).T
        store_first((w1f, w1hm, w1lo), w1f[...] - dot(keys_t, dh8[...]))

    def prepare(c, step):
        w1f, w1hm, w1lo, w2f, w2hm, w2lo, b1r, b2r, zb, cor, dh8, hps, slope, d3r = chains[c]
        x = jnp.concatenate([load(c, 2, step), load(c, 0, jnp.minimum(step + 1, n_steps - 1))], axis=0)
        zb[...] = base(x, w1hm, w1lo, b1r)
        cor[...] = correction(x, load(c, 0, step))

    def second_layer(c):
        w1f, w1hm, w1lo, w2f, w2hm, w2lo, b1r, b2r, zb, cor, dh8, hps, slope, d3r = chains[c]
        return dot_t(hps[...], w2hm[...]), dot_t(hps[:2 * MINI], w2lo[...])

    def normalised(c, r, yl):
        n2 = 2 * MINI
        r = r[:, :dim] + r[:, dim:]
        yc = r[:n2] + r[n2:2 * n2] + r[2 * n2:] + yl + chains[c][7][...]
        rstd = lax.rsqrt(jnp.mean(yc * yc, axis=1, keepdims=True) + EPS)
        return yc * rstd, rstd

    def residual(c, step, r, yl):
        w1f, w1hm, w1lo, w2f, w2hm, w2lo, b1r, b2r, zb, cor, dh8, hps, slope, d3r = chains[c]
        before = jnp.maximum(step - 1, 0)
        xhat, rstd = normalised(c, r, yl)
        store_out(c, before, load(c, 2, before).astype(F32) + gain * xhat[:MINI] + bias)
        xk = xhat[MINI:]
        dx = (load(c, 0, step).astype(F32) + gain * xk + bias - load(c, 1, step).astype(F32)) * ((2.0 * factor) * gain)
        m1 = jnp.mean(dx, axis=1, keepdims=True)
        m2 = jnp.mean(dx * xk, axis=1, keepdims=True)
        dy = rstd[MINI:] * (dx - m1 - xk * m2)
        d3r[...] = jnp.concatenate(split3(dy), axis=0)
        b2r[...] = b2r[...] - jnp.sum(dy, axis=0, keepdims=True)

    def back_dots(c):
        w1f, w1hm, w1lo, w2f, w2hm, w2lo, b1r, b2r, zb, cor, dh8, hps, slope, d3r = chains[c]
        d3 = d3r[...]
        return dot(jnp.concatenate([d3, d3], axis=1), w2hm[...]), dot(d3[:MINI], w2lo[...])

    def back_end(c, e, el):
        w1f, w1hm, w1lo, w2f, w2hm, w2lo, b1r, b2r, zb, cor, dh8, hps, slope, d3r = chains[c]
        dh = (e[:MINI] + e[MINI:2 * MINI] + e[2 * MINI:] + el) * slope[...]
        dh8[:6 * MINI] = jnp.concatenate(six(split3(dh)), axis=0)
        b1r[...] = b1r[...] - jnp.sum(dh, axis=0, keepdims=True)

    def update_second(c):
        w1f, w1hm, w1lo, w2f, w2hm, w2lo, b1r, b2r, zb, cor, dh8, hps, slope, d3r = chains[c]
        parts = [hps[(2 * i + 1) * MINI:(2 * i + 2) * MINI] for i in range(3)]
        hk8 = jnp.concatenate(six(parts) + [zeros32], axis=0)
        dyp = [d3r[i * MINI:(i + 1) * MINI] for i in range(3)]
        dy_t = jnp.concatenate(six_other(dyp) + [jnp.zeros((2 * MINI, dim), BF16)], axis=0).T
        store_first((w2f, w2hm, w2lo), w2f[...] - dot(dy_t, hk8))

    def one_step(step):
        ev = [c for c in range(n_chains) if c % 2 == 0]
        od = [c for c in range(n_chains) if c % 2 == 1]
        before = jnp.maximum(step - 1, 0)
        held = {}
        for part in ORDER:
            for c in (ev if part[0] == "A" else od):
                name = part[2:]
                if name == "corr":
                    held[c, "z"] = hidden_in(c)
                elif name == "gelu":
                    activate(c, held[c, "z"])
                elif name == "w1":
                    update_first(c, before if part[0] == "A" else step)
                elif name == "base":
                    prepare(c, step)
                elif name == "y":
                    held[c, "y"] = second_layer(c)
                elif name == "ln":
                    residual(c, step, *held[c, "y"])
                elif name == "dh":
                    held[c, "e"] = back_dots(c)
                elif name == "end":
                    back_end(c, *held[c, "e"])
                elif name == "w2":
                    update_second(c)

    for c in range(n_chains):
        w1f, w1hm, w1lo, w2f, w2hm, w2lo, b1r, b2r, zb, cor, dh8, hps, slope, d3r = chains[c]
        store_first((w1f, w1hm, w1lo), w1[...])
        w2t = w2[...].T
        w2t = w2t - jnp.mean(w2t, axis=0, keepdims=True)
        store_first((w2f, w2hm, w2lo), w2t)
        b1r[...] = b_one[pl.ds(head, 1), :]
        b2 = b_two[pl.ds(head, 1), :]
        b2r[...] = b2 - jnp.mean(b2, axis=1, keepdims=True)
        dh8[...] = jnp.zeros_like(dh8)
        cor[...] = jnp.zeros_like(cor)
        hps[...] = jnp.zeros_like(hps)
        d3r[...] = jnp.zeros_like(d3r)

    wait_piece(0)
    for c in range(n_chains):
        w1f, w1hm, w1lo, w2f, w2hm, w2lo, b1r, b2r, zb, cor, dh8, hps, slope, d3r = chains[c]
        zb[...] = base(jnp.concatenate([load(c, 2, 0), load(c, 0, 0)], axis=0), w1hm, w1lo, b1r)
        if c % 2 == 1:
            activate(c, hidden_in(c))

    def take_turns(running):
        while running:
            running = [g for g in running if next(g, 1) is None]

    def body(step, carry):
        after = step + 1

        @pl.when((lax.rem(after, per_piece) == 0) & (after < n_steps))
        def _():
            wait_piece(after // per_piece)

        send_some(1, (2, 3, 0), step == 0)
        send_some(1, (1,), step == PACE)
        send_some(2, (2, 1, 3, 0), step == (me - 1) * PACE)
        send_some(3, (2, 1, 3, 0), step == (me - half + 1) * PACE)

        number = (step - 1) // per_piece - 1
        finished = (lax.rem(step, per_piece) == 1) & (step > per_piece)

        @pl.when(finished & (number < first_direct * n_sp))
        def _():
            send_out(number, False)

        @pl.when(finished & (number >= first_direct * n_sp))
        def _():
            send_out(number, True)

        period = n_sp * per_piece
        since_share = step - SHARE_LAG - per_piece * my_turn
        since_group = step - GROUP_LAG - per_piece * my_turn

        @pl.when((since_share >= 0) & (since_share < first_direct * period) & (lax.rem(since_share, period) == 0))
        def _():
            share_group(since_share // period)

        @pl.when(step == GROUP_LAG)
        def _():
            for off in range(1, n_hp):
                w_copy(off).wait_recv()
            pl.semaphore_wait(ready_sem, n_hp - 1)

        @pl.when((since_group >= 0) & (since_group < first_direct * period) & (lax.rem(since_group, period) == 0))
        def _():
            group = since_group // period
            others = gath.at[group, pl.ds(0, n_all - n_sp)]
            pltpu.make_async_copy(others, others, srecv_sem.at[group]).wait()
            make_group(group)

        one_step(step)
        return carry

    lax.fori_loop(0, n_steps, body, 0)

    def last_output(c):
        if c % 2 == 0:
            z = hidden_in(c)
            update_second(c)
            yield
            activate(c, z)
        yield
        r, yl = second_layer(c)
        yield
        xhat, _ = normalised(c, r, yl)
        store_out(c, n_steps - 1, load(c, 2, n_steps - 1).astype(F32) + gain * xhat[:MINI] + bias)

    take_turns([last_output(c) for c in range(n_chains)])
    send_out(n_groups * n_sp - 1, True)
    for group in range(first_direct, n_groups):
        spread = gath.at[group, pl.ds(0, n_all - 1)]
        pltpu.make_async_copy(spread, spread, orecv_sem.at[group]).wait()
        make_group(group)

    for q in range(n_pieces):
        @pl.when(q != lax.rem(my_turn, n_pieces))
        def _():
            pltpu.make_async_copy(resb.at[q], resb.at[q], rrecv_sem.at[q]).wait()

        for b in range(batch):
            res[b, q * PIECE:(q + 1) * PIECE] = resb[q, b]

    for group in range(n_groups):
        owner, q, copy = result_copy(group)

        @pl.when(owner != me)
        def _():
            copy.wait_send()

    sent = outb.at[pl.ds(0, first_direct * (n_sp - 1))]
    pltpu.make_async_copy(sent, sent, osend_sem.at[0]).wait()
    sent = gath.at[pl.ds(0, DIRECT), pl.ds(0, n_all - 1)]
    pltpu.make_async_copy(sent, sent, osend_sem.at[1]).wait()
    shared = gath.at[pl.ds(0, first_direct), pl.ds(0, n_all - n_sp)]
    pltpu.make_async_copy(shared, shared, ssend_sem).wait()
    for off in range(1, n_hp):
        w_copy(off).wait_send()
    for which, (cond, size) in enumerate(kinds):
        @pl.when(cond)
        def _():
            for copy in copies(which, (0, 1, 2, 3)):
                copy.wait_send()


def run(n_hp, n_sp, tokens, theta_k, theta_v, theta_q, w_out, w_one, w_two, b_one, b_two, gammas, betas, rates):
    batch, block, model = tokens.shape
    heads, dim, hid = w_one.shape
    n_chains = heads * batch // n_sp
    assert batch % n_chains == 0 and heads % 2 == 0 and block % PIECE == 0
    n_pieces = block // PIECE
    n_all = n_hp * n_sp
    n_groups = n_pieces
    cols = model // n_hp
    any_ref, vmem = pl.BlockSpec(memory_space=pl.ANY), pl.BlockSpec(memory_space=pltpu.VMEM)
    dma, v = pltpu.SemaphoreType.DMA, pltpu.VMEM
    per_chain = [
        v((dim, hid), F32), v((2 * dim, hid), BF16), v((dim, hid), BF16),
        v((dim, hid), F32), v((2 * dim, hid), BF16), v((dim, hid), BF16),
        v((1, hid), F32), v((1, dim), F32), v((2 * MINI, hid), F32),
        v((2 * MINI, 8 * MINI), BF16), v((8 * MINI, hid), BF16),
        v((6 * MINI, hid), BF16), v((MINI, hid), F32), v((3 * MINI, dim), BF16),
    ]
    assert len(per_chain) == CHAIN_REFS
    scratch = [
        v((batch * block, model), BF16), v((2, model, heads // 2 * 3 * dim), BF16), v((n_hp * heads * dim, cols), BF16),
        v((n_sp, n_pieces, n_chains, 3, PIECE, dim), BF16), v((n_sp, n_pieces, n_chains, 3, PIECE, dim), BF16),
        v((n_sp * n_pieces, n_chains, PIECE, dim), BF16), v((n_groups, n_all, n_chains, PIECE, dim), BF16),
        v((n_groups, batch, PIECE, cols), BF16), v((n_pieces, batch, PIECE, cols), BF16),
        v((dim, hid), F32), v((hid, dim), F32),
        dma((batch + 3 * heads + 3,)), dma((n_sp, n_pieces)), dma((n_sp, n_pieces)), dma((n_hp,)), dma((n_hp,)), dma((2,)),
        dma((n_groups,)), dma, dma((n_groups,)), dma((n_groups,)), dma((n_pieces,)), pltpu.SemaphoreType.REGULAR,
    ] + per_chain * n_chains
    return pl.pallas_call(
        functools.partial(ttt_kernel, n_hp, n_sp, n_chains),
        out_shape=jax.ShapeDtypeStruct((batch, block, cols), BF16),
        in_specs=[any_ref] * 7 + [vmem] * 4 + [pl.BlockSpec(memory_space=pltpu.SMEM)],
        out_specs=vmem,
        scratch_shapes=scratch,
        compiler_params=pltpu.CompilerParams(collective_id=0, has_side_effects=True),
    )(tokens, theta_k, theta_v, theta_q, w_out, w_one, w_two, b_one, b_two, gammas, betas, rates)


def solution(mesh):
    n_sp = mesh.shape["sp"]
    n_hp = mesh.shape["hp"]

    def local_fn(tokens, theta_q, theta_k, theta_v, w_out, w_one, b_one, w_two, b_two, ln_gamma, ln_beta, inner_lr):
        return run(n_hp, n_sp, tokens, theta_k, theta_v, theta_q, w_out, w_one, w_two, b_one, b_two, ln_gamma, ln_beta, inner_lr)

    head_spec = P("hp", None)
    cube_spec = P("hp", None, None)
    col_spec = P(None, "hp")
    return jax.shard_map(local_fn, mesh=mesh, in_specs=(P("dp", "sp", None), col_spec, col_spec, col_spec, head_spec, cube_spec, head_spec, cube_spec, head_spec, head_spec, head_spec, P("hp")), out_specs=P("dp", "sp", "hp"), check_vma=False)
```

```python
import functools

import jax
import jax.numpy as jnp
from jax import lax
from jax.experimental import pallas as pl
from jax.experimental.pallas import tpu as pltpu
from jax.sharding import PartitionSpec as P

MINI = 16
EPS = 1e-6
GELU_A = 0.7978845608028654
GELU_B = 0.044715
F32 = jnp.float32
BF16 = jnp.bfloat16


def split3(x):
    high = x.astype(BF16)
    rest = x - high.astype(F32)
    mid = rest.astype(BF16)
    low = (rest - mid.astype(F32)).astype(BF16)
    return high, mid, low


def dot(a, b):
    return jnp.dot(a, b, preferred_element_type=F32)


def dot_t(a, b):
    return lax.dot_general(a, b, (((1,), (1,)), ((), ())), preferred_element_type=F32)


def six(parts):
    high, mid, low = parts
    return [high, mid, low, high, mid, high]


def six_other(parts):
    high, mid, low = parts
    return [high, high, high, mid, mid, low]


MESH = pl.DeviceIdType.MESH
PIECE = 2 * MINI
CHAIN_REFS = 14
TURNS = [[2, 1], [3, 0]]
ORDER = ("B w1s", "B y", "A w2f", "A corr", "A gelu", "A w1f", "A y", "B base", "B ln", "B dh", "A base", "B end",
         "A ln", "B w2f", "B corr", "B w1", "A dh", "B gelu", "A end")
PACE = 4
SHARE_LAG = 16
GROUP_LAG = 40
DIRECT = 3
W_STEP = 0


def ttt_kernel(n_hp, n_sp, n_chains, tokens, theta_k, theta_v, theta_q, w_out, w_one, w_two, b_one, b_two, gammas, betas, rates,
               res, tok, theta, wcols, kvq, send, outb, gath, made, resb, w1, w2, in_sem, send_sem, recv_sem, wsend_sem,
               wrecv_sem, osend_sem, orecv_sem, ssend_sem, srecv_sem, rsend_sem, rrecv_sem, ready_sem, *scr):
    batch, block, model = tokens.shape
    heads, dim, hid = w_one.shape
    n_pieces = block // PIECE
    per_block = block // MINI
    per_piece = PIECE // MINI
    n_steps = n_sp * per_block
    cols = model // n_hp
    rows = heads * dim
    per_head = batch // n_chains
    my_hp, me = lax.axis_index("hp"), lax.axis_index("sp")
    linear = my_hp * n_sp + me
    n_all = n_hp * n_sp
    head = me // per_head
    chains = [scr[i * CHAIN_REFS:(i + 1) * CHAIN_REFS] for i in range(n_chains)]
    factor = rates[head] / MINI
    gain, bias = gammas[pl.ds(head, 1), :], betas[pl.ds(head, 1), :]

    def head_of(turn):
        return lax.rem(head + turn, heads)

    barrier = pltpu.get_barrier_semaphore()
    for off in range(1, n_sp):
        pl.semaphore_signal(barrier, inc=1, device_id={"sp": lax.rem(me + off, n_sp)}, device_id_type=MESH)
    for off in range(1, n_hp):
        pl.semaphore_signal(barrier, inc=1, device_id={"hp": lax.rem(my_hp + off, n_hp)}, device_id_type=MESH)

    loads = []

    def fetch(src, dst):
        copy = pltpu.make_async_copy(src, dst, in_sem.at[len(loads)])
        copy.start()
        loads.append(copy)

    for b in range(batch):
        fetch(tokens.at[b], tok.at[pl.ds(b * block, block)])
    for r, pair in enumerate(TURNS):
        for u, turn in enumerate(pair):
            where = pl.ds(pl.multiple_of(head_of(turn) * dim, dim), dim)
            for i, part in enumerate((theta_k, theta_v, theta_q)):
                fetch(part.at[:, where], theta.at[r, :, pl.ds((u * 3 + i) * dim, dim)])
    fetch(w_one.at[head], w1)
    fetch(w_two.at[head], w2)
    mine = pl.ds(pl.multiple_of(my_hp * cols, cols), cols)
    my_rows = pl.ds(pl.multiple_of(my_hp * rows, rows), rows)
    fetch(w_out.at[:, mine], wcols.at[my_rows])

    half = n_sp // 2
    chip, core = me // 2, lax.rem(me, 2)

    def kvq_copy(delta, other, q, size):
        dest = lax.rem(chip + delta, half) * 2 + lax.rem(core + other, 2)
        return pltpu.make_async_remote_copy(
            src_ref=send.at[dest, pl.ds(q, size)], dst_ref=kvq.at[me, pl.ds(q, size)], send_sem=send_sem.at[2 * delta + other, q],
            recv_sem=recv_sem.at[me, q], device_id={"sp": dest}, device_id_type=MESH)

    kinds = [(me == 0, 1), (me == 1, 1), ((me > 1) & (me < half), 2), (me >= half, n_pieces)]

    def copies(which, deltas):
        size = kinds[which][1]
        return [kvq_copy(delta, other, q, size) for q in range(0, n_pieces, size) for delta in deltas for other in (0, 1)
                if delta + other > 0]

    def send_some(which, deltas, gate):
        @pl.when(kinds[which][0] & gate)
        def _():
            for copy in copies(which, deltas):
                copy.start()

    done = 0
    for r, pair in enumerate(TURNS):
        upto = batch + (r + 1) * 3 * len(pair)
        for copy in loads[done:upto]:
            copy.wait()
        done = upto
        p = dot(tok[...], theta[r]).astype(BF16)
        for u, turn in enumerate(pair):
            for b in range(batch):
                dest = head_of(turn) * per_head + b // n_chains
                for i in range(3):
                    tile = p[b * block:(b + 1) * block, (u * 3 + i) * dim:(u * 3 + i + 1) * dim]
                    for q in range(n_pieces):
                        send[dest, q, b % n_chains, i] = tile[q * PIECE:(q + 1) * PIECE]
        if r == 0:
            pl.semaphore_wait(barrier, n_sp + n_hp - 2)
            for off in range(1, n_hp):
                pl.semaphore_signal(ready_sem, inc=1, device_id={"hp": lax.rem(my_hp + off, n_hp)}, device_id_type=MESH)
        send_some(0, pair, me == 0)
    for copy in loads[done:]:
        copy.wait()
    kvq[me] = send[me]

    def wait_piece(number):
        src, q = number // n_pieces, lax.rem(number, n_pieces)

        def wait(size):
            pltpu.make_async_remote_copy(
                src_ref=send.at[0, pl.ds(q, size)], dst_ref=kvq.at[src, pl.ds(q, size)], send_sem=send_sem.at[0, q],
                recv_sem=recv_sem.at[src, q], device_id={"sp": src}, device_id_type=MESH).wait_recv()

        @pl.when((src != me) & (src < 2))
        def _():
            wait(1)

        @pl.when((src != me) & (src > 1) & (src < half) & (lax.rem(q, 2) == 0))
        def _():
            wait(2)

        @pl.when((src != me) & (src >= half) & (q == 0))
        def _():
            wait(n_pieces)

    def w_copy(off):
        dest = lax.rem(my_hp + off, n_hp)
        return pltpu.make_async_remote_copy(
            src_ref=w_out.at[:, pl.ds(pl.multiple_of(dest * cols, cols), cols)], dst_ref=wcols.at[my_rows],
            send_sem=wsend_sem.at[off], recv_sem=wrecv_sem.at[off], device_id={"hp": dest}, device_id_type=MESH)

    for off in range(1, n_hp):
        w_copy(off).start()

    def worker_of(turn):
        return lax.rem(turn, half) * 2 + turn // half

    my_turn = me // 2 + half * lax.rem(me, 2)
    n_groups = n_steps // per_piece // n_sp
    last = n_groups - 1
    first_direct = n_groups - DIRECT
    my_slots = pl.ds(pl.multiple_of(my_hp * n_sp, n_sp), n_sp)

    def send_out(number, spread, rows=pl.ds(0, PIECE)):
        group, dest = number // n_sp, worker_of(lax.rem(number, n_sp))

        def start(off):
            target = lax.rem(my_hp + off, n_hp)
            pltpu.make_async_remote_copy(
                src_ref=outb.at[number, :, rows], dst_ref=gath.at[group, linear, :, rows], send_sem=osend_sem.at[int(spread)],
                recv_sem=orecv_sem.at[group], device_id={"hp": target, "sp": dest},
                device_id_type=MESH).start()

        if spread:
            for off in range(1, n_hp):
                start(off)

        @pl.when(dest != me)
        def _():
            start(0)

        @pl.when(dest == me)
        def _():
            gath[group, linear, :, rows] = outb[number, :, rows]

    def share_copy(group, off):
        return pltpu.make_async_remote_copy(
            src_ref=gath.at[group, my_slots], dst_ref=gath.at[group, my_slots], send_sem=ssend_sem, recv_sem=srecv_sem.at[group],
            device_id={"hp": lax.rem(my_hp + off, n_hp)}, device_id_type=MESH)

    def share_group(group):
        others = gath.at[group, pl.ds(0, n_sp - 1)]
        pltpu.make_async_copy(others, others, orecv_sem.at[group]).wait()
        for off in range(1, n_hp):
            share_copy(group, off).start()

    def result_copy(group):
        number = group * n_sp + my_turn
        owner, q = number // n_pieces, lax.rem(number, n_pieces)
        return owner, q, pltpu.make_async_remote_copy(
            src_ref=made.at[group], dst_ref=resb.at[q], send_sem=rsend_sem.at[group], recv_sem=rrecv_sem.at[q],
            device_id={"sp": owner}, device_id_type=MESH)

    def make_group(group):
        left = []
        for one in range(n_hp * heads):
            chain = [one * batch + b for b in range(batch)]
            left.append(jnp.concatenate([gath[group, c // n_chains, c % n_chains] for c in chain], axis=0))
        made[group] = dot(jnp.concatenate(left, axis=1), wcols[...]).astype(BF16).reshape(batch, PIECE, cols)
        owner, q, copy = result_copy(group)

        @pl.when(owner != me)
        def _():
            copy.start()

        @pl.when(owner == me)
        def _():
            resb[q] = made[group]

    def load(chain, which, step):
        piece = lax.rem(step, per_block)
        return kvq[step // per_block, piece // per_piece, chain, which, pl.ds(pl.multiple_of(lax.rem(piece, per_piece) * MINI, MINI), MINI), :]

    def store_out(chain, step, value):
        outb[step // per_piece, chain, pl.ds(pl.multiple_of(lax.rem(step, per_piece) * MINI, MINI), MINI), :] = value.astype(BF16)

    def spread_parts(full, pair, low_part):
        store_parts((full, pair, low_part), full[...])

    def store_parts(refs, value):
        full, pair, low_part = refs
        high, mid, low = split3(value)
        pair[:dim] = high
        pair[dim:] = mid
        low_part[...] = low

    def correction(x, keys):
        rep = jnp.concatenate([keys] * 8, axis=0)
        a = dot_t(x, rep) + 1.0
        high, mid, low = split3(a)
        lane = lax.broadcasted_iota(jnp.int32, a.shape, 1)
        part = jnp.where(lane < 3 * MINI, high.astype(F32), jnp.where(lane < 5 * MINI, mid.astype(F32), low.astype(F32)))
        return jnp.where(lane < 6 * MINI, part, 0.0).astype(BF16)

    def base(x, w1hm, w1lo, b1r):
        return dot(jnp.concatenate([x, x], axis=1), w1hm[...]) + dot(x, w1lo[...]) + b1r[...]

    zeros32 = jnp.zeros((2 * MINI, hid), BF16)

    def hidden_in(c):
        return chains[c][8][...] - dot(chains[c][9][...], chains[c][10][...])

    def activate(c, z):
        w1f, w1hm, w1lo, w2f, w2hm, w2lo, b1r, b2r, zb, cor, dh8, hps, slope, d3r = chains[c]
        z2 = z * z
        t = jnp.tanh(z * (GELU_A + (GELU_A * GELU_B) * z2))
        cdf = 0.5 + 0.5 * t
        hps[...] = jnp.concatenate(split3(z * cdf), axis=0)
        zk, z2k, tk = z[MINI:], z2[MINI:], t[MINI:]
        slope[...] = cdf[MINI:] + (0.5 * zk * (1.0 - tk * tk)) * (GELU_A + (3.0 * GELU_A * GELU_B) * z2k)

    def update_first(c, step):
        w1f, w1hm, w1lo, w2f, w2hm, w2lo, b1r, b2r, zb, cor, dh8, hps, slope, d3r = chains[c]
        keys_t = jnp.concatenate([load(c, 0, step)] * 3 + [jnp.zeros((5 * MINI, dim), BF16)], axis=0).T
        return (w1f, w1hm, w1lo), w1f[...] - dot(keys_t, dh8[...])

    def prepare(c, step):
        w1f, w1hm, w1lo, w2f, w2hm, w2lo, b1r, b2r, zb, cor, dh8, hps, slope, d3r = chains[c]
        x = jnp.concatenate([load(c, 2, step), load(c, 0, jnp.minimum(step + 1, n_steps - 1))], axis=0)
        zb[...] = base(x, w1hm, w1lo, b1r)
        cor[...] = correction(x, load(c, 0, step))

    def second_layer(c):
        w1f, w1hm, w1lo, w2f, w2hm, w2lo, b1r, b2r, zb, cor, dh8, hps, slope, d3r = chains[c]
        return dot_t(hps[...], w2hm[...]), dot_t(hps[:2 * MINI], w2lo[...])

    def normalised(c, r, yl):
        n2 = 2 * MINI
        r = r[:, :dim] + r[:, dim:]
        yc = r[:n2] + r[n2:2 * n2] + r[2 * n2:] + yl + chains[c][7][...]
        rstd = lax.rsqrt(jnp.mean(yc * yc, axis=1, keepdims=True) + EPS)
        return yc * rstd, rstd

    def residual(c, step, r, yl):
        w1f, w1hm, w1lo, w2f, w2hm, w2lo, b1r, b2r, zb, cor, dh8, hps, slope, d3r = chains[c]
        before = jnp.maximum(step - 1, 0)
        xhat, rstd = normalised(c, r, yl)
        store_out(c, before, load(c, 2, before).astype(F32) + gain * xhat[:MINI] + bias)
        xk = xhat[MINI:]
        dx = (load(c, 0, step).astype(F32) + gain * xk + bias - load(c, 1, step).astype(F32)) * ((2.0 * factor) * gain)
        m1 = jnp.mean(dx, axis=1, keepdims=True)
        m2 = jnp.mean(dx * xk, axis=1, keepdims=True)
        dy = rstd[MINI:] * (dx - m1 - xk * m2)
        d3r[...] = jnp.concatenate(split3(dy), axis=0)
        b2r[...] = b2r[...] - jnp.sum(dy, axis=0, keepdims=True)

    def back_dots(c):
        w1f, w1hm, w1lo, w2f, w2hm, w2lo, b1r, b2r, zb, cor, dh8, hps, slope, d3r = chains[c]
        d3 = d3r[...]
        return dot(jnp.concatenate([d3, d3], axis=1), w2hm[...]), dot(d3[:MINI], w2lo[...])

    def back_end(c, e, el):
        w1f, w1hm, w1lo, w2f, w2hm, w2lo, b1r, b2r, zb, cor, dh8, hps, slope, d3r = chains[c]
        dh = (e[:MINI] + e[MINI:2 * MINI] + e[2 * MINI:] + el) * slope[...]
        dh8[:6 * MINI] = jnp.concatenate(six(split3(dh)), axis=0)
        b1r[...] = b1r[...] - jnp.sum(dh, axis=0, keepdims=True)

    def update_second(c):
        w1f, w1hm, w1lo, w2f, w2hm, w2lo, b1r, b2r, zb, cor, dh8, hps, slope, d3r = chains[c]
        parts = [hps[(2 * i + 1) * MINI:(2 * i + 2) * MINI] for i in range(3)]
        hk8 = jnp.concatenate(six(parts) + [zeros32], axis=0)
        dyp = [d3r[i * MINI:(i + 1) * MINI] for i in range(3)]
        dy_t = jnp.concatenate(six_other(dyp) + [jnp.zeros((2 * MINI, dim), BF16)], axis=0).T
        return (w2f, w2hm, w2lo), w2f[...] - dot(dy_t, hk8)

    def one_step(step):
        ev = [c for c in range(n_chains) if c % 2 == 0]
        od = [c for c in range(n_chains) if c % 2 == 1]
        before = jnp.maximum(step - 1, 0)
        held = {}
        for part in ORDER:
            for c in (ev if part[0] == "A" else od):
                name = part[2:]
                if name == "corr":
                    held[c, "z"] = hidden_in(c)
                elif name == "gelu":
                    activate(c, held[c, "z"])
                elif name in ("w1", "w1f"):
                    refs, value = update_first(c, before if part[0] == "A" else step)
                    refs[0][...] = value
                    if name == "w1f":
                        store_parts(refs, value)
                elif name == "w1s":
                    spread_parts(*chains[c][0:3])
                elif name == "w2s":
                    spread_parts(*chains[c][3:6])
                elif name == "base":
                    prepare(c, step)
                elif name == "y":
                    held[c, "y"] = second_layer(c)
                elif name == "ln":
                    residual(c, step, *held[c, "y"])
                elif name == "dh":
                    held[c, "e"] = back_dots(c)
                elif name == "end":
                    back_end(c, *held[c, "e"])
                elif name in ("w2", "w2f"):
                    refs, value = update_second(c)
                    refs[0][...] = value
                    if name == "w2f":
                        store_parts(refs, value)

    for c in range(n_chains):
        w1f, w1hm, w1lo, w2f, w2hm, w2lo, b1r, b2r, zb, cor, dh8, hps, slope, d3r = chains[c]
        w1f[...] = w1[...]
        spread_parts(w1f, w1hm, w1lo)
        w2t = w2[...].T
        w2f[...] = w2t - jnp.mean(w2t, axis=0, keepdims=True)
        spread_parts(w2f, w2hm, w2lo)
        b1r[...] = b_one[pl.ds(head, 1), :]
        b2 = b_two[pl.ds(head, 1), :]
        b2r[...] = b2 - jnp.mean(b2, axis=1, keepdims=True)
        dh8[...] = jnp.zeros_like(dh8)
        cor[...] = jnp.zeros_like(cor)
        hps[...] = jnp.zeros_like(hps)
        d3r[...] = jnp.zeros_like(d3r)

    wait_piece(0)
    for c in range(n_chains):
        w1f, w1hm, w1lo, w2f, w2hm, w2lo, b1r, b2r, zb, cor, dh8, hps, slope, d3r = chains[c]
        zb[...] = base(jnp.concatenate([load(c, 2, 0), load(c, 0, 0)], axis=0), w1hm, w1lo, b1r)
        if c % 2 == 1:
            activate(c, hidden_in(c))

    def take_turns(running):
        while running:
            running = [g for g in running if next(g, 1) is None]

    def body(step, carry):
        after = step + 1

        @pl.when((lax.rem(after, per_piece) == 0) & (after < n_steps))
        def _():
            wait_piece(after // per_piece)

        send_some(1, (2, 3, 0), step == 0)
        send_some(1, (1,), step == PACE)
        send_some(2, (2, 1, 3, 0), step == (me - 1) * PACE)
        send_some(3, (2, 1, 3, 0), step == (me - half + 1) * PACE)

        @pl.when(step == per_block)
        def _():
            pl.semaphore_wait(ready_sem, n_hp - 1)

        number = (step - 1) // per_piece - 1
        finished = (lax.rem(step, per_piece) == 1) & (step > per_piece)

        @pl.when(finished & (number < first_direct * n_sp))
        def _():
            send_out(number, False)

        @pl.when(finished & (number >= first_direct * n_sp))
        def _():
            send_out(number, True)

        period = n_sp * per_piece
        since_share = step - SHARE_LAG - per_piece * my_turn
        since_group = step - GROUP_LAG - per_piece * my_turn

        @pl.when((since_share >= 0) & (since_share < first_direct * period) & (lax.rem(since_share, period) == 0))
        def _():
            share_group(since_share // period)

        @pl.when(step == GROUP_LAG)
        def _():
            for off in range(1, n_hp):
                w_copy(off).wait_recv()

        @pl.when((since_group >= 0) & (since_group < first_direct * period) & (lax.rem(since_group, period) == 0))
        def _():
            group = since_group // period
            others = gath.at[group, pl.ds(0, n_all - n_sp)]
            pltpu.make_async_copy(others, others, srecv_sem.at[group]).wait()
            make_group(group)

        one_step(step)
        return carry

    lax.fori_loop(0, n_steps, body, 0)

    def last_output(c):
        if c % 2 == 0:
            z = hidden_in(c)
            store_parts(*update_second(c))
            yield
            activate(c, z)
        yield
        r, yl = second_layer(c)
        yield
        xhat, _ = normalised(c, r, yl)
        store_out(c, n_steps - 1, load(c, 2, n_steps - 1).astype(F32) + gain * xhat[:MINI] + bias)

    send_out(n_groups * n_sp - 1, True, pl.ds(0, PIECE - MINI))
    take_turns([last_output(c) for c in range(n_chains)])
    send_out(n_groups * n_sp - 1, True, pl.ds(PIECE - MINI, MINI))
    for group in range(first_direct, n_groups):
        spread = gath.at[group, pl.ds(0, n_all - 1)]
        pltpu.make_async_copy(spread, spread, orecv_sem.at[group]).wait()
        make_group(group)

    for q in range(n_pieces):
        @pl.when(q != lax.rem(my_turn, n_pieces))
        def _():
            pltpu.make_async_copy(resb.at[q], resb.at[q], rrecv_sem.at[q]).wait()

        for b in range(batch):
            res[b, q * PIECE:(q + 1) * PIECE] = resb[q, b]

    for group in range(n_groups):
        owner, q, copy = result_copy(group)

        @pl.when(owner != me)
        def _():
            copy.wait_send()

    sent = outb.at[pl.ds(0, first_direct * (n_sp - 1))]
    pltpu.make_async_copy(sent, sent, osend_sem.at[0]).wait()
    sent = gath.at[pl.ds(0, DIRECT), pl.ds(0, n_all - 1)]
    pltpu.make_async_copy(sent, sent, osend_sem.at[1]).wait()
    shared = gath.at[pl.ds(0, first_direct), pl.ds(0, n_all - n_sp)]
    pltpu.make_async_copy(shared, shared, ssend_sem).wait()
    for off in range(1, n_hp):
        w_copy(off).wait_send()
    for which, (cond, size) in enumerate(kinds):
        @pl.when(cond)
        def _():
            for copy in copies(which, (0, 1, 2, 3)):
                copy.wait_send()


def run(n_hp, n_sp, tokens, theta_k, theta_v, theta_q, w_out, w_one, w_two, b_one, b_two, gammas, betas, rates):
    batch, block, model = tokens.shape
    heads, dim, hid = w_one.shape
    n_chains = heads * batch // n_sp
    assert batch % n_chains == 0 and heads % 2 == 0 and block % PIECE == 0
    n_pieces = block // PIECE
    n_all = n_hp * n_sp
    n_groups = n_pieces
    cols = model // n_hp
    any_ref, vmem = pl.BlockSpec(memory_space=pl.ANY), pl.BlockSpec(memory_space=pltpu.VMEM)
    dma, v = pltpu.SemaphoreType.DMA, pltpu.VMEM
    per_chain = [
        v((dim, hid), F32), v((2 * dim, hid), BF16), v((dim, hid), BF16),
        v((dim, hid), F32), v((2 * dim, hid), BF16), v((dim, hid), BF16),
        v((1, hid), F32), v((1, dim), F32), v((2 * MINI, hid), F32),
        v((2 * MINI, 8 * MINI), BF16), v((8 * MINI, hid), BF16),
        v((6 * MINI, hid), BF16), v((MINI, hid), F32), v((3 * MINI, dim), BF16),
    ]
    assert len(per_chain) == CHAIN_REFS
    scratch = [
        v((batch * block, model), BF16), v((2, model, heads // 2 * 3 * dim), BF16), v((n_hp * heads * dim, cols), BF16),
        v((n_sp, n_pieces, n_chains, 3, PIECE, dim), BF16), v((n_sp, n_pieces, n_chains, 3, PIECE, dim), BF16),
        v((n_sp * n_pieces, n_chains, PIECE, dim), BF16), v((n_groups, n_all, n_chains, PIECE, dim), BF16),
        v((n_groups, batch, PIECE, cols), BF16), v((n_pieces, batch, PIECE, cols), BF16),
        v((dim, hid), F32), v((hid, dim), F32),
        dma((batch + 3 * heads + 3,)), dma((n_sp, n_pieces)), dma((n_sp, n_pieces)), dma((n_hp,)), dma((n_hp,)), dma((2,)),
        dma((n_groups,)), dma, dma((n_groups,)), dma((n_groups,)), dma((n_pieces,)), pltpu.SemaphoreType.REGULAR,
    ] + per_chain * n_chains
    return pl.pallas_call(
        functools.partial(ttt_kernel, n_hp, n_sp, n_chains),
        out_shape=jax.ShapeDtypeStruct((batch, block, cols), BF16),
        in_specs=[any_ref] * 7 + [vmem] * 4 + [pl.BlockSpec(memory_space=pltpu.SMEM)],
        out_specs=vmem,
        scratch_shapes=scratch,
        compiler_params=pltpu.CompilerParams(collective_id=0, has_side_effects=True),
    )(tokens, theta_k, theta_v, theta_q, w_out, w_one, w_two, b_one, b_two, gammas, betas, rates)


def solution(mesh):
    n_sp = mesh.shape["sp"]
    n_hp = mesh.shape["hp"]

    def local_fn(tokens, theta_q, theta_k, theta_v, w_out, w_one, b_one, w_two, b_two, ln_gamma, ln_beta, inner_lr):
        return run(n_hp, n_sp, tokens, theta_k, theta_v, theta_q, w_out, w_one, w_two, b_one, b_two, ln_gamma, ln_beta, inner_lr)

    head_spec = P("hp", None)
    cube_spec = P("hp", None, None)
    col_spec = P(None, "hp")
    return jax.shard_map(local_fn, mesh=mesh, in_specs=(P("dp", "sp", None), col_spec, col_spec, col_spec, head_spec, cube_spec, head_spec, cube_spec, head_spec, head_spec, head_spec, P("hp")), out_specs=P("dp", "sp", "hp"), check_vma=False)
```

```python
import functools

import jax
import jax.numpy as jnp
from jax import lax
from jax.experimental import pallas as pl
from jax.experimental.pallas import tpu as pltpu
from jax.sharding import PartitionSpec as P

MINI = 16
EPS = 1e-6
GELU_A = 0.7978845608028654
GELU_B = 0.044715
F32 = jnp.float32
BF16 = jnp.bfloat16


def split3(x):
    high = x.astype(BF16)
    rest = x - high.astype(F32)
    mid = rest.astype(BF16)
    low = (rest - mid.astype(F32)).astype(BF16)
    return high, mid, low


def dot(a, b):
    return jnp.dot(a, b, preferred_element_type=F32)


def dot_t(a, b):
    return lax.dot_general(a, b, (((1,), (1,)), ((), ())), preferred_element_type=F32)


def six(parts):
    high, mid, low = parts
    return [high, mid, low, high, mid, high]


def six_other(parts):
    high, mid, low = parts
    return [high, high, high, mid, mid, low]


MESH = pl.DeviceIdType.MESH
PIECE = 2 * MINI
CHAIN_REFS = 14
TURNS = [[2, 1], [3, 0]]
ORDER = ("B w1s", "B y", "A w2f", "A corr", "A gelu", "A w1f", "A y", "B base", "B ln", "B dh", "A base", "B end",
         "A ln", "B w2f", "B corr", "B w1", "A dh", "B gelu", "A end")
PACE = 4
SHARE_LAG = 16
GROUP_LAG = 40
DIRECT = 3
W_STEP = 0


def ttt_kernel(n_hp, n_sp, n_chains, tokens, theta_k, theta_v, theta_q, w_out, w_one, w_two, b_one, b_two, gammas, betas, rates,
               res, tok, theta, wcols, kvq, send, outb, gath, made, resb, w1, w2, in_sem, send_sem, recv_sem, wsend_sem,
               wrecv_sem, osend_sem, orecv_sem, ssend_sem, srecv_sem, rsend_sem, rrecv_sem, ready_sem, *scr):
    batch, block, model = tokens.shape
    heads, dim, hid = w_one.shape
    n_pieces = block // PIECE
    per_block = block // MINI
    per_piece = PIECE // MINI
    n_steps = n_sp * per_block
    cols = model // n_hp
    rows = heads * dim
    per_head = batch // n_chains
    my_hp, me = lax.axis_index("hp"), lax.axis_index("sp")
    linear = my_hp * n_sp + me
    n_all = n_hp * n_sp
    head = me // per_head
    chains = [scr[i * CHAIN_REFS:(i + 1) * CHAIN_REFS] for i in range(n_chains)]
    factor = rates[head] / MINI
    gain, bias = gammas[pl.ds(head, 1), :], betas[pl.ds(head, 1), :]

    def head_of(turn):
        return lax.rem(head + turn, heads)

    loads = []

    def fetch(src, dst):
        copy = pltpu.make_async_copy(src, dst, in_sem.at[len(loads)])
        copy.start()
        loads.append(copy)

    for b in range(batch):
        fetch(tokens.at[b], tok.at[pl.ds(b * block, block)])
    for r, pair in enumerate(TURNS):
        for u, turn in enumerate(pair):
            where = pl.ds(pl.multiple_of(head_of(turn) * dim, dim), dim)
            for i, part in enumerate((theta_k, theta_v, theta_q)):
                fetch(part.at[:, where], theta.at[r, :, pl.ds((u * 3 + i) * dim, dim)])
    fetch(w_one.at[head], w1)
    fetch(w_two.at[head], w2)
    mine = pl.ds(pl.multiple_of(my_hp * cols, cols), cols)
    my_rows = pl.ds(pl.multiple_of(my_hp * rows, rows), rows)
    fetch(w_out.at[:, mine], wcols.at[my_rows])

    barrier = pltpu.get_barrier_semaphore()
    for off in range(1, n_sp):
        pl.semaphore_signal(barrier, inc=1, device_id={"sp": lax.rem(me + off, n_sp)}, device_id_type=MESH)
    for off in range(1, n_hp):
        pl.semaphore_signal(barrier, inc=1, device_id={"hp": lax.rem(my_hp + off, n_hp)}, device_id_type=MESH)

    half = n_sp // 2
    chip, core = me // 2, lax.rem(me, 2)

    def kvq_copy(delta, other, q, size):
        dest = lax.rem(chip + delta, half) * 2 + lax.rem(core + other, 2)
        return pltpu.make_async_remote_copy(
            src_ref=send.at[dest, pl.ds(q, size)], dst_ref=kvq.at[me, pl.ds(q, size)], send_sem=send_sem.at[2 * delta + other, q],
            recv_sem=recv_sem.at[me, q], device_id={"sp": dest}, device_id_type=MESH)

    kinds = [(me == 0, 1), (me == 1, 1), ((me > 1) & (me < half), 2), (me >= half, n_pieces)]

    def copies(which, deltas):
        size = kinds[which][1]
        return [kvq_copy(delta, other, q, size) for q in range(0, n_pieces, size) for delta in deltas for other in (0, 1)
                if delta + other > 0]

    def send_some(which, deltas, gate):
        @pl.when(kinds[which][0] & gate)
        def _():
            for copy in copies(which, deltas):
                copy.start()

    done = 0
    for r, pair in enumerate(TURNS):
        upto = batch + (r + 1) * 3 * len(pair)
        for copy in loads[done:upto]:
            copy.wait()
        done = upto
        p = dot(tok[...], theta[r]).astype(BF16)
        for u, turn in enumerate(pair):
            for b in range(batch):
                dest = head_of(turn) * per_head + b // n_chains
                for i in range(3):
                    tile = p[b * block:(b + 1) * block, (u * 3 + i) * dim:(u * 3 + i + 1) * dim]
                    for q in range(n_pieces):
                        send[dest, q, b % n_chains, i] = tile[q * PIECE:(q + 1) * PIECE]
        if r == 0:
            pl.semaphore_wait(barrier, n_sp + n_hp - 2)
            for off in range(1, n_hp):
                pl.semaphore_signal(ready_sem, inc=1, device_id={"hp": lax.rem(my_hp + off, n_hp)}, device_id_type=MESH)
        send_some(0, pair, me == 0)
    for copy in loads[done:]:
        copy.wait()
    kvq[me] = send[me]

    def wait_piece(number):
        src, q = number // n_pieces, lax.rem(number, n_pieces)

        def wait(size):
            pltpu.make_async_remote_copy(
                src_ref=send.at[0, pl.ds(q, size)], dst_ref=kvq.at[src, pl.ds(q, size)], send_sem=send_sem.at[0, q],
                recv_sem=recv_sem.at[src, q], device_id={"sp": src}, device_id_type=MESH).wait_recv()

        @pl.when((src != me) & (src < 2))
        def _():
            wait(1)

        @pl.when((src != me) & (src > 1) & (src < half) & (lax.rem(q, 2) == 0))
        def _():
            wait(2)

        @pl.when((src != me) & (src >= half) & (q == 0))
        def _():
            wait(n_pieces)

    def w_copy(off):
        dest = lax.rem(my_hp + off, n_hp)
        return pltpu.make_async_remote_copy(
            src_ref=w_out.at[:, pl.ds(pl.multiple_of(dest * cols, cols), cols)], dst_ref=wcols.at[my_rows],
            send_sem=wsend_sem.at[off], recv_sem=wrecv_sem.at[off], device_id={"hp": dest}, device_id_type=MESH)

    for off in range(1, n_hp):
        w_copy(off).start()

    def worker_of(turn):
        return lax.rem(turn, half) * 2 + turn // half

    my_turn = me // 2 + half * lax.rem(me, 2)
    n_groups = n_steps // per_piece // n_sp
    last = n_groups - 1
    first_direct = n_groups - DIRECT
    my_slots = pl.ds(pl.multiple_of(my_hp * n_sp, n_sp), n_sp)

    def send_out(number, spread, rows=pl.ds(0, PIECE)):
        group, dest = number // n_sp, worker_of(lax.rem(number, n_sp))

        def start(off):
            target = lax.rem(my_hp + off, n_hp)
            pltpu.make_async_remote_copy(
                src_ref=outb.at[number, :, rows], dst_ref=gath.at[group, linear, :, rows], send_sem=osend_sem.at[int(spread)],
                recv_sem=orecv_sem.at[group], device_id={"hp": target, "sp": dest},
                device_id_type=MESH).start()

        if spread:
            for off in range(1, n_hp):
                start(off)

        @pl.when(dest != me)
        def _():
            start(0)

        @pl.when(dest == me)
        def _():
            gath[group, linear, :, rows] = outb[number, :, rows]

    def share_copy(group, off):
        return pltpu.make_async_remote_copy(
            src_ref=gath.at[group, my_slots], dst_ref=gath.at[group, my_slots], send_sem=ssend_sem, recv_sem=srecv_sem.at[group],
            device_id={"hp": lax.rem(my_hp + off, n_hp)}, device_id_type=MESH)

    def share_group(group):
        others = gath.at[group, pl.ds(0, n_sp - 1)]
        pltpu.make_async_copy(others, others, orecv_sem.at[group]).wait()
        for off in range(1, n_hp):
            share_copy(group, off).start()

    def result_copy(group):
        number = group * n_sp + my_turn
        owner, q = number // n_pieces, lax.rem(number, n_pieces)
        return owner, q, pltpu.make_async_remote_copy(
            src_ref=made.at[group], dst_ref=resb.at[q], send_sem=rsend_sem.at[group], recv_sem=rrecv_sem.at[q],
            device_id={"sp": owner}, device_id_type=MESH)

    def make_group(group):
        left = []
        for one in range(n_hp * heads):
            chain = [one * batch + b for b in range(batch)]
            left.append(jnp.concatenate([gath[group, c // n_chains, c % n_chains] for c in chain], axis=0))
        made[group] = dot(jnp.concatenate(left, axis=1), wcols[...]).astype(BF16).reshape(batch, PIECE, cols)
        owner, q, copy = result_copy(group)

        @pl.when(owner != me)
        def _():
            copy.start()

        @pl.when(owner == me)
        def _():
            resb[q] = made[group]

    def load(chain, which, step):
        piece = lax.rem(step, per_block)
        return kvq[step // per_block, piece // per_piece, chain, which, pl.ds(pl.multiple_of(lax.rem(piece, per_piece) * MINI, MINI), MINI), :]

    def store_out(chain, step, value):
        outb[step // per_piece, chain, pl.ds(pl.multiple_of(lax.rem(step, per_piece) * MINI, MINI), MINI), :] = value.astype(BF16)

    def spread_parts(full, pair, low_part):
        store_parts((full, pair, low_part), full[...])

    def store_parts(refs, value):
        full, pair, low_part = refs
        high, mid, low = split3(value)
        pair[:dim] = high
        pair[dim:] = mid
        low_part[...] = low

    def correction(x, keys):
        rep = jnp.concatenate([keys] * 8, axis=0)
        a = dot_t(x, rep) + 1.0
        high, mid, low = split3(a)
        lane = lax.broadcasted_iota(jnp.int32, a.shape, 1)
        part = jnp.where(lane < 3 * MINI, high.astype(F32), jnp.where(lane < 5 * MINI, mid.astype(F32), low.astype(F32)))
        return jnp.where(lane < 6 * MINI, part, 0.0).astype(BF16)

    def base(x, w1hm, w1lo, b1r):
        return dot(jnp.concatenate([x, x], axis=1), w1hm[...]) + dot(x, w1lo[...]) + b1r[...]

    zeros32 = jnp.zeros((2 * MINI, hid), BF16)

    def hidden_in(c):
        return chains[c][8][...] - dot(chains[c][9][...], chains[c][10][...])

    def activate(c, z):
        w1f, w1hm, w1lo, w2f, w2hm, w2lo, b1r, b2r, zb, cor, dh8, hps, slope, d3r = chains[c]
        z2 = z * z
        t = jnp.tanh(z * (GELU_A + (GELU_A * GELU_B) * z2))
        cdf = 0.5 + 0.5 * t
        hps[...] = jnp.concatenate(split3(z * cdf), axis=0)
        zk, z2k, tk = z[MINI:], z2[MINI:], t[MINI:]
        slope[...] = cdf[MINI:] + (0.5 * zk * (1.0 - tk * tk)) * (GELU_A + (3.0 * GELU_A * GELU_B) * z2k)

    def update_first(c, step):
        w1f, w1hm, w1lo, w2f, w2hm, w2lo, b1r, b2r, zb, cor, dh8, hps, slope, d3r = chains[c]
        keys_t = jnp.concatenate([load(c, 0, step)] * 3 + [jnp.zeros((5 * MINI, dim), BF16)], axis=0).T
        return (w1f, w1hm, w1lo), w1f[...] - dot(keys_t, dh8[...])

    def prepare(c, step):
        w1f, w1hm, w1lo, w2f, w2hm, w2lo, b1r, b2r, zb, cor, dh8, hps, slope, d3r = chains[c]
        x = jnp.concatenate([load(c, 2, step), load(c, 0, jnp.minimum(step + 1, n_steps - 1))], axis=0)
        zb[...] = base(x, w1hm, w1lo, b1r)
        cor[...] = correction(x, load(c, 0, step))

    def second_layer(c):
        w1f, w1hm, w1lo, w2f, w2hm, w2lo, b1r, b2r, zb, cor, dh8, hps, slope, d3r = chains[c]
        return dot_t(hps[...], w2hm[...]), dot_t(hps[:2 * MINI], w2lo[...])

    def normalised(c, r, yl):
        n2 = 2 * MINI
        r = r[:, :dim] + r[:, dim:]
        yc = r[:n2] + r[n2:2 * n2] + r[2 * n2:] + yl + chains[c][7][...]
        rstd = lax.rsqrt(jnp.mean(yc * yc, axis=1, keepdims=True) + EPS)
        return yc * rstd, rstd

    def residual(c, step, r, yl):
        w1f, w1hm, w1lo, w2f, w2hm, w2lo, b1r, b2r, zb, cor, dh8, hps, slope, d3r = chains[c]
        before = jnp.maximum(step - 1, 0)
        xhat, rstd = normalised(c, r, yl)
        store_out(c, before, load(c, 2, before).astype(F32) + gain * xhat[:MINI] + bias)
        xk = xhat[MINI:]
        dx = (load(c, 0, step).astype(F32) + gain * xk + bias - load(c, 1, step).astype(F32)) * ((2.0 * factor) * gain)
        m1 = jnp.mean(dx, axis=1, keepdims=True)
        m2 = jnp.mean(dx * xk, axis=1, keepdims=True)
        dy = rstd[MINI:] * (dx - m1 - xk * m2)
        d3r[...] = jnp.concatenate(split3(dy), axis=0)
        b2r[...] = b2r[...] - jnp.sum(dy, axis=0, keepdims=True)

    def back_dots(c):
        w1f, w1hm, w1lo, w2f, w2hm, w2lo, b1r, b2r, zb, cor, dh8, hps, slope, d3r = chains[c]
        d3 = d3r[...]
        return dot(jnp.concatenate([d3, d3], axis=1), w2hm[...]), dot(d3[:MINI], w2lo[...])

    def back_end(c, e, el):
        w1f, w1hm, w1lo, w2f, w2hm, w2lo, b1r, b2r, zb, cor, dh8, hps, slope, d3r = chains[c]
        dh = (e[:MINI] + e[MINI:2 * MINI] + e[2 * MINI:] + el) * slope[...]
        dh8[:6 * MINI] = jnp.concatenate(six(split3(dh)), axis=0)
        b1r[...] = b1r[...] - jnp.sum(dh, axis=0, keepdims=True)

    def update_second(c):
        w1f, w1hm, w1lo, w2f, w2hm, w2lo, b1r, b2r, zb, cor, dh8, hps, slope, d3r = chains[c]
        parts = [hps[(2 * i + 1) * MINI:(2 * i + 2) * MINI] for i in range(3)]
        hk8 = jnp.concatenate(six(parts) + [zeros32], axis=0)
        dyp = [d3r[i * MINI:(i + 1) * MINI] for i in range(3)]
        dy_t = jnp.concatenate(six_other(dyp) + [jnp.zeros((2 * MINI, dim), BF16)], axis=0).T
        return (w2f, w2hm, w2lo), w2f[...] - dot(dy_t, hk8)

    def one_step(step):
        ev = [c for c in range(n_chains) if c % 2 == 0]
        od = [c for c in range(n_chains) if c % 2 == 1]
        before = jnp.maximum(step - 1, 0)
        held = {}
        for part in ORDER:
            for c in (ev if part[0] == "A" else od):
                name = part[2:]
                if name == "corr":
                    held[c, "z"] = hidden_in(c)
                elif name == "gelu":
                    activate(c, held[c, "z"])
                elif name in ("w1", "w1f"):
                    refs, value = update_first(c, before if part[0] == "A" else step)
                    refs[0][...] = value
                    if name == "w1f":
                        store_parts(refs, value)
                elif name == "w1s":
                    spread_parts(*chains[c][0:3])
                elif name == "w2s":
                    spread_parts(*chains[c][3:6])
                elif name == "base":
                    prepare(c, step)
                elif name == "y":
                    held[c, "y"] = second_layer(c)
                elif name == "ln":
                    residual(c, step, *held[c, "y"])
                elif name == "dh":
                    held[c, "e"] = back_dots(c)
                elif name == "end":
                    back_end(c, *held[c, "e"])
                elif name in ("w2", "w2f"):
                    refs, value = update_second(c)
                    refs[0][...] = value
                    if name == "w2f":
                        store_parts(refs, value)

    for c in range(n_chains):
        w1f, w1hm, w1lo, w2f, w2hm, w2lo, b1r, b2r, zb, cor, dh8, hps, slope, d3r = chains[c]
        w1f[...] = w1[...]
        spread_parts(w1f, w1hm, w1lo)
        w2t = w2[...].T
        w2f[...] = w2t - jnp.mean(w2t, axis=0, keepdims=True)
        spread_parts(w2f, w2hm, w2lo)
        b1r[...] = b_one[pl.ds(head, 1), :]
        b2 = b_two[pl.ds(head, 1), :]
        b2r[...] = b2 - jnp.mean(b2, axis=1, keepdims=True)
        dh8[...] = jnp.zeros_like(dh8)
        cor[...] = jnp.zeros_like(cor)
        hps[...] = jnp.zeros_like(hps)
        d3r[...] = jnp.zeros_like(d3r)

    wait_piece(0)
    for c in range(n_chains):
        w1f, w1hm, w1lo, w2f, w2hm, w2lo, b1r, b2r, zb, cor, dh8, hps, slope, d3r = chains[c]
        zb[...] = base(jnp.concatenate([load(c, 2, 0), load(c, 0, 0)], axis=0), w1hm, w1lo, b1r)
        if c % 2 == 1:
            activate(c, hidden_in(c))

    def take_turns(running):
        while running:
            running = [g for g in running if next(g, 1) is None]

    def body(step, carry):
        after = step + 1

        @pl.when((lax.rem(after, per_piece) == 0) & (after < n_steps))
        def _():
            wait_piece(after // per_piece)

        send_some(1, (2, 3, 0), step == 0)
        send_some(1, (1,), step == PACE)
        send_some(2, (2, 1, 3, 0), step == (me - 1) * PACE)
        send_some(3, (2, 1, 3, 0), step == (me - half + 1) * PACE)

        @pl.when(step == per_block)
        def _():
            pl.semaphore_wait(ready_sem, n_hp - 1)

        number = (step - 1) // per_piece - 1
        finished = (lax.rem(step, per_piece) == 1) & (step > per_piece)

        @pl.when(finished & (number < first_direct * n_sp))
        def _():
            send_out(number, False)

        @pl.when(finished & (number >= first_direct * n_sp))
        def _():
            send_out(number, True)

        period = n_sp * per_piece
        since_share = step - SHARE_LAG - per_piece * my_turn
        since_group = step - GROUP_LAG - per_piece * my_turn

        @pl.when((since_share >= 0) & (since_share < first_direct * period) & (lax.rem(since_share, period) == 0))
        def _():
            share_group(since_share // period)

        @pl.when(step == GROUP_LAG)
        def _():
            for off in range(1, n_hp):
                w_copy(off).wait_recv()

        @pl.when((since_group >= 0) & (since_group < first_direct * period) & (lax.rem(since_group, period) == 0))
        def _():
            group = since_group // period
            others = gath.at[group, pl.ds(0, n_all - n_sp)]
            pltpu.make_async_copy(others, others, srecv_sem.at[group]).wait()
            make_group(group)

        one_step(step)
        return carry

    lax.fori_loop(0, n_steps, body, 0)

    def last_output(c):
        if c % 2 == 0:
            z = hidden_in(c)
            store_parts(*update_second(c))
            yield
            activate(c, z)
        yield
        r, yl = second_layer(c)
        yield
        xhat, _ = normalised(c, r, yl)
        store_out(c, n_steps - 1, load(c, 2, n_steps - 1).astype(F32) + gain * xhat[:MINI] + bias)

    send_out(n_groups * n_sp - 1, True, pl.ds(0, PIECE - MINI))
    take_turns([last_output(c) for c in range(n_chains)])
    send_out(n_groups * n_sp - 1, True, pl.ds(PIECE - MINI, MINI))
    for group in range(first_direct, n_groups):
        spread = gath.at[group, pl.ds(0, n_all - 1)]
        pltpu.make_async_copy(spread, spread, orecv_sem.at[group]).wait()
        make_group(group)

    for q in range(n_pieces):
        @pl.when(q != lax.rem(my_turn, n_pieces))
        def _():
            pltpu.make_async_copy(resb.at[q], resb.at[q], rrecv_sem.at[q]).wait()

        for b in range(batch):
            res[b, q * PIECE:(q + 1) * PIECE] = resb[q, b]

    for group in range(n_groups):
        owner, q, copy = result_copy(group)

        @pl.when(owner != me)
        def _():
            copy.wait_send()

    sent = outb.at[pl.ds(0, first_direct * (n_sp - 1))]
    pltpu.make_async_copy(sent, sent, osend_sem.at[0]).wait()
    sent = gath.at[pl.ds(0, DIRECT), pl.ds(0, n_all - 1)]
    pltpu.make_async_copy(sent, sent, osend_sem.at[1]).wait()
    shared = gath.at[pl.ds(0, first_direct), pl.ds(0, n_all - n_sp)]
    pltpu.make_async_copy(shared, shared, ssend_sem).wait()
    for off in range(1, n_hp):
        w_copy(off).wait_send()
    for which, (cond, size) in enumerate(kinds):
        @pl.when(cond)
        def _():
            for copy in copies(which, (0, 1, 2, 3)):
                copy.wait_send()


def run(n_hp, n_sp, tokens, theta_k, theta_v, theta_q, w_out, w_one, w_two, b_one, b_two, gammas, betas, rates):
    batch, block, model = tokens.shape
    heads, dim, hid = w_one.shape
    n_chains = heads * batch // n_sp
    assert batch % n_chains == 0 and heads % 2 == 0 and block % PIECE == 0
    n_pieces = block // PIECE
    n_all = n_hp * n_sp
    n_groups = n_pieces
    cols = model // n_hp
    any_ref, vmem = pl.BlockSpec(memory_space=pl.ANY), pl.BlockSpec(memory_space=pltpu.VMEM)
    dma, v = pltpu.SemaphoreType.DMA, pltpu.VMEM
    per_chain = [
        v((dim, hid), F32), v((2 * dim, hid), BF16), v((dim, hid), BF16),
        v((dim, hid), F32), v((2 * dim, hid), BF16), v((dim, hid), BF16),
        v((1, hid), F32), v((1, dim), F32), v((2 * MINI, hid), F32),
        v((2 * MINI, 8 * MINI), BF16), v((8 * MINI, hid), BF16),
        v((6 * MINI, hid), BF16), v((MINI, hid), F32), v((3 * MINI, dim), BF16),
    ]
    assert len(per_chain) == CHAIN_REFS
    scratch = [
        v((batch * block, model), BF16), v((2, model, heads // 2 * 3 * dim), BF16), v((n_hp * heads * dim, cols), BF16),
        v((n_sp, n_pieces, n_chains, 3, PIECE, dim), BF16), v((n_sp, n_pieces, n_chains, 3, PIECE, dim), BF16),
        v((n_sp * n_pieces, n_chains, PIECE, dim), BF16), v((n_groups, n_all, n_chains, PIECE, dim), BF16),
        v((n_groups, batch, PIECE, cols), BF16), v((n_pieces, batch, PIECE, cols), BF16),
        v((dim, hid), F32), v((hid, dim), F32),
        dma((batch + 3 * heads + 3,)), dma((n_sp, n_pieces)), dma((n_sp, n_pieces)), dma((n_hp,)), dma((n_hp,)), dma((2,)),
        dma((n_groups,)), dma, dma((n_groups,)), dma((n_groups,)), dma((n_pieces,)), pltpu.SemaphoreType.REGULAR,
    ] + per_chain * n_chains
    return pl.pallas_call(
        functools.partial(ttt_kernel, n_hp, n_sp, n_chains),
        out_shape=jax.ShapeDtypeStruct((batch, block, cols), BF16),
        in_specs=[any_ref] * 7 + [vmem] * 4 + [pl.BlockSpec(memory_space=pltpu.SMEM)],
        out_specs=vmem,
        scratch_shapes=scratch,
        compiler_params=pltpu.CompilerParams(collective_id=0, has_side_effects=True),
    )(tokens, theta_k, theta_v, theta_q, w_out, w_one, w_two, b_one, b_two, gammas, betas, rates)


def solution(mesh):
    n_sp = mesh.shape["sp"]
    n_hp = mesh.shape["hp"]

    def local_fn(tokens, theta_q, theta_k, theta_v, w_out, w_one, b_one, w_two, b_two, ln_gamma, ln_beta, inner_lr):
        return run(n_hp, n_sp, tokens, theta_k, theta_v, theta_q, w_out, w_one, w_two, b_one, b_two, ln_gamma, ln_beta, inner_lr)

    head_spec = P("hp", None)
    cube_spec = P("hp", None, None)
    col_spec = P(None, "hp")
    return jax.shard_map(local_fn, mesh=mesh, in_specs=(P("dp", "sp", None), col_spec, col_spec, col_spec, head_spec, cube_spec, head_spec, cube_spec, head_spec, head_spec, head_spec, P("hp")), out_specs=P("dp", "sp", "hp"), check_vma=False)
```
